8 devices in a mesh: part: 1 (over z), row: 2 (over y), col: 4 (over x, core).
Axes of the slice: x: 2, y: 2, z: 1, core: 2. Of those that a mesh axis runs over, the one named last changes fastest.
Arguments:
- counts: bfloat16 [8192, 16384], P(('part', 'row'), 'col')
- w_init: float32 [8192, 256], P(('part', 'row'))
- h_init: float32 [256, 16384], P(None, ('part', 'col'))
Outputs:
- output 1: float32 [8192, 256], P(('part', 'row'))
- output 2: float32 [256, 16384], P(None, ('part', 'col'))
All inputs are finite; a program needn't handle non-finite values.
Results may differ from the reference program's by a relative error of at most 0.001.
Values are sent between devices in bfloat16 or wider.
A program may use at most 1 GiB of HBM per device.

```python
import jax
import jax.numpy as jnp
from jax import lax

ROW_DEVS = 2
COL_DEVS = 4
DOC_DEV = 4096
WORD_DEV = 4096
TOPICS = 256
SWEEPS = 4
LATENT = 8

DOCS = ROW_DEVS * DOC_DEV
WORDS = COL_DEVS * WORD_DEV
EPS = 1e-6


def setup_inputs(seed: int = 0, part: int = 0) -> dict:
    base_key = jax.random.fold_in(jax.random.key(seed), part)
    sub_keys = jax.random.split(base_key, 7)
    w_true = jax.random.randint(sub_keys[0], (DOCS, LATENT), 0, 4)
    h_true = jax.random.randint(sub_keys[1], (LATENT, WORDS), 0, 4)
    noise_int = jax.random.randint(sub_keys[2], (DOCS, WORDS), -3, 4)
    counts = jnp.clip(jnp.dot(w_true, h_true) + noise_int, 0, 256).astype(jnp.bfloat16)
    init_scale = 4.0 * TOPICS ** -0.5
    w_gain = 2.0 ** jax.random.uniform(sub_keys[3], (1, TOPICS), jnp.float32, -1.0, 1.0)
    h_gain = 2.0 ** jax.random.uniform(sub_keys[4], (TOPICS, 1), jnp.float32, -1.0, 1.0)
    w_init = jax.random.uniform(sub_keys[5], (DOCS, TOPICS), jnp.float32, 0.5, 1.5) * w_gain * init_scale
    h_init = jax.random.uniform(sub_keys[6], (TOPICS, WORDS), jnp.float32, 0.5, 1.5) * h_gain * init_scale
    return {'counts': counts, 'w_init': w_init.astype(jnp.float32), 'h_init': h_init.astype(jnp.float32)}


def ratio_block(c_blk, w_blk, h_blk):
    z_blk = jnp.dot(w_blk, h_blk, preferred_element_type=jnp.float32)
    return (c_blk.astype(jnp.float32) / (z_blk + EPS)).astype(jnp.bfloat16)


def update_w(w_cur, h_cur, c_by_row):
    w_blocks = w_cur.astype(jnp.bfloat16).reshape(ROW_DEVS, DOC_DEV, TOPICS)
    h_blocks = h_cur.astype(jnp.bfloat16).reshape(TOPICS, COL_DEVS, WORD_DEV).transpose(1, 0, 2)

    def one_row(row_items):
        w_blk, c_row = row_items

        def col_step(running, col_items):
            h_blk, c_blk = col_items
            q_blk = ratio_block(c_blk, w_blk, h_blk)
            return running + jnp.dot(q_blk, h_blk.T, preferred_element_type=jnp.float32), None

        total, _ = lax.scan(col_step, jnp.zeros((DOC_DEV, TOPICS), jnp.float32), (h_blocks, c_row))
        return total

    a_w = lax.map(one_row, (w_blocks, c_by_row)).reshape(DOCS, TOPICS)
    s_h = jnp.sum(h_cur, axis=1)
    return w_cur * a_w / s_h[None, :]


def update_h(w_cur, h_cur, c_by_col):
    w_blocks = w_cur.astype(jnp.bfloat16).reshape(ROW_DEVS, DOC_DEV, TOPICS)
    h_blocks = h_cur.astype(jnp.bfloat16).reshape(TOPICS, COL_DEVS, WORD_DEV).transpose(1, 0, 2)

    def one_col(col_items):
        h_blk, c_col = col_items

        def row_step(running, row_items):
            w_blk, c_blk = row_items
            q_blk = ratio_block(c_blk, w_blk, h_blk)
            return running + jnp.dot(w_blk.T, q_blk, preferred_element_type=jnp.float32), None

        total, _ = lax.scan(row_step, jnp.zeros((TOPICS, WORD_DEV), jnp.float32), (w_blocks, c_col))
        return total

    a_h = lax.map(one_col, (h_blocks, c_by_col)).transpose(1, 0, 2).reshape(TOPICS, WORDS)
    s_w = jnp.sum(w_cur, axis=0)
    return h_cur * a_h / s_w[:, None]


def reference(counts, w_init, h_init):
    c_blocks = counts.reshape(ROW_DEVS, DOC_DEV, COL_DEVS, WORD_DEV)
    c_by_row = c_blocks.transpose(0, 2, 1, 3)
    c_by_col = c_blocks.transpose(2, 0, 1, 3)

    def one_sweep(state, unused):
        w_cur, h_cur = state
        w_cur = update_w(w_cur, h_cur, c_by_row)
        h_cur = update_h(w_cur, h_cur, c_by_col)
        return (w_cur, h_cur), None

    (w_out, h_out), _ = lax.scan(one_sweep, (w_init, h_init), None, length=SWEEPS)
    return (w_out, h_out)
```

```python
import functools

import jax
import jax.numpy as jnp
from jax import lax
from jax.experimental import pallas as pl
from jax.experimental.pallas import tpu as pltpu
from jax.sharding import PartitionSpec as P

SWEEPS = 4
EPS = 1e-6
ND = 8
NV = 8
LANES = 128
MESH = pl.DeviceIdType.MESH
F32 = jnp.float32
BF16 = jnp.bfloat16


def kernel(
    rows, cols, c_hbm, w_hbm, h_hbm, w_out, h_out,
    c_v, w_bf, w_t, h_bf, h_t, w_f, h_f, a_w, a_h, r_a, r_x, r_y,
    sw_acc, sw_slots, sw_col, sh_acc, sh_part, sh_slots, sh_row,
    load_sem, c_sem,
    a_send, a_recv, x_send, x_recv, g_send, g_recv, p_send, p_recv, q_send, q_recv,
    y_send, y_recv, z_send, z_recv, sw_send, sw_recv, sh_send, sh_recv,
    wo_send, wo_recv, ho_send, ho_recv, ow_sem, oh_sem,
):
    docs, words = c_v.shape
    topics = w_bf.shape[1]
    dt, vt, kh = docs // ND, words // NV, topics // 2
    half, quarter = dt // 2, dt // 4
    n_dev = rows * cols
    y, i = lax.axis_index("row"), lax.axis_index("col")
    x, core = i // 2, i % 2
    me = y * cols + i
    partner = {"col": x * 2 + (1 - core)}
    across = {"col": (1 - x) * 2 + core}
    above = {"row": 1 - y}

    def peer(step):
        other = (me + step) % n_dev
        return {"row": other // cols, "col": other % cols}

    def rows_at(start, size):
        return pl.ds(pl.multiple_of(start, size), size)

    def remote(src, dst, send, recv, device):
        return pltpu.make_async_remote_copy(
            src_ref=src, dst_ref=dst, send_sem=send, recv_sem=recv, device_id=device, device_id_type=MESH)

    def mine(d):
        return rows_at(d * dt + core * half + x * quarter, quarter)

    def theirs(d):
        return rows_at(d * dt + core * half + (1 - x) * quarter, quarter)

    def copy_a(d):
        return remote(a_w.at[rows_at(d * dt + (1 - core) * half, half)], r_a.at[rows_at(d * half, half)],
                      a_send.at[d], a_recv.at[d], partner)

    def copy_x(d):
        return remote(a_w.at[theirs(d)], r_x.at[rows_at(d * quarter, quarter)], x_send.at[d], x_recv.at[d], across)

    def copy_g(d):
        return remote(w_bf.at[mine(d)], w_bf.at[mine(d)], g_send.at[d], g_recv.at[d], across)

    def copy_p(d):
        return remote(w_bf.at[mine(d)], w_bf.at[mine(d)], p_send.at[d], p_recv.at[d], partner)

    def copy_q(d):
        return remote(w_bf.at[theirs(d)], w_bf.at[theirs(d)], q_send.at[d], q_recv.at[d], partner)

    own_k, other_k = rows_at(y * kh, kh), rows_at((1 - y) * kh, kh)

    def words_at(v):
        return rows_at(v * vt, vt)

    def copy_y(v):
        return remote(a_h.at[other_k, words_at(v)], r_y.at[:, words_at(v)], y_send.at[v], y_recv.at[v], above)

    def copy_z(v):
        return remote(h_bf.at[own_k, words_at(v)], h_bf.at[own_k, words_at(v)], z_send.at[v], z_recv.at[v], above)

    def copy_sw(step):
        return remote(sw_acc, sw_slots.at[me], sw_send.at[step - 1], sw_recv.at[step - 1], peer(step))

    def copy_sh(step):
        return remote(sh_part, sh_slots.at[me], sh_send.at[step - 1], sh_recv.at[step - 1], peer(step))

    def copy_wo(d, step):
        k = d * (cols - 1) + step - 1
        return remote(w_f.at[rows_at(d * quarter, quarter)], w_out.at[mine(d)], wo_send.at[k], wo_recv.at[k],
                      {"col": (i + step) % cols})

    def copy_ho(v):
        return remote(h_f.at[:, words_at(v)], h_out.at[own_k, words_at(v)], ho_send.at[v], ho_recv.at[v], above)

    def out_w(d):
        return pltpu.make_async_copy(w_f.at[rows_at(d * quarter, quarter)], w_out.at[mine(d)], ow_sem.at[d])

    def out_h(v):
        return pltpu.make_async_copy(h_f.at[:, words_at(v)], h_out.at[own_k, words_at(v)], oh_sem.at[v])

    def load_c(d):
        return pltpu.make_async_copy(c_hbm.at[rows_at(d * dt, dt)], c_v.at[rows_at(d * dt, dt)], c_sem.at[d])

    def each(count, body):
        def step(n, carry):
            body(n)
            return carry
        lax.fori_loop(0, count, step, 0)

    def ratio(d, v):
        z = jnp.dot(w_bf[rows_at(d * dt, dt), :], h_bf[:, words_at(v)], preferred_element_type=F32)
        return (c_v[rows_at(d * dt, dt), words_at(v)].astype(F32) / (z + EPS)).astype(BF16)

    def w_tile(d, v):
        part = jnp.dot(ratio(d, v), h_t[words_at(v), :], preferred_element_type=F32)
        held = a_w[rows_at(d * dt, dt), :]
        a_w[rows_at(d * dt, dt), :] = jnp.where(v == 0, 0.0, held) + part

    def h_tile(d, v):
        part = jnp.dot(w_t[...], ratio(d, v), preferred_element_type=F32)
        held = a_h[:, words_at(v)]
        a_h[:, words_at(v)] = jnp.where(d == 0, 0.0, held) + part

    def fold_lanes(block):
        total = block[:, :LANES]
        for g in range(1, block.shape[1] // LANES):
            total = total + block[:, g * LANES:(g + 1) * LANES]
        return total

    def send_sh():
        sh_part[...] = jnp.sum(sh_acc[...].T.reshape(LANES // 8, 8, kh), axis=0)
        sh_slots[me] = sh_part[...]
        for step in range(1, n_dev):
            copy_sh(step).start()

    def take_sh():
        for step in range(1, n_dev):
            copy_sh(step).wait()
        for r in range(rows):
            total = sh_slots[r * cols]
            for n in range(1, cols):
                total = total + sh_slots[r * cols + n]
            sh_row[:, r * kh:(r + 1) * kh] = jnp.broadcast_to(jnp.sum(total, axis=0, keepdims=True), (8, kh))

    def send_sw():
        sw_slots[me] = sw_acc[...]
        for step in range(1, n_dev):
            copy_sw(step).start()

    def take_sw():
        for step in range(1, n_dev):
            copy_sw(step).wait()
        total = sw_slots[0]
        for n in range(1, n_dev):
            total = total + sw_slots[n]
        total = jnp.sum(total, axis=0, keepdims=True)
        own = jnp.where(y == 0, total[:, :kh], total[:, kh:])
        sw_col[...] = jnp.broadcast_to(own, (LANES, kh)).T

    load_h = pltpu.make_async_copy(h_hbm, a_h, load_sem.at[0])
    load_w = pltpu.make_async_copy(w_hbm, a_w, load_sem.at[1])
    load_h.start()
    load_w.start()
    for d in range(ND):
        load_c(d).start()
    barrier = pltpu.get_barrier_semaphore()
    for step in range(1, n_dev):
        pl.semaphore_signal(barrier, inc=1, device_id=peer(step), device_id_type=MESH)
    pl.semaphore_wait(barrier, n_dev - 1)

    load_h.wait()
    sh_acc[...] = jnp.zeros_like(sh_acc)

    def start_h(v):
        h_bf[:, words_at(v)] = a_h[:, words_at(v)].astype(BF16)
        own = a_h[own_k, words_at(v)]
        h_f[:, words_at(v)] = own
        sh_acc[...] += fold_lanes(own)
        h_t[words_at(v), :] = h_bf[:, words_at(v)].T

    each(NV, start_h)
    send_sh()
    load_w.wait()

    def start_w(d):
        w_bf[rows_at(d * dt, dt), :] = a_w[rows_at(d * dt, dt), :].astype(BF16)
        w_f[rows_at(d * quarter, quarter), :] = a_w[mine(d), :]

    each(ND, start_w)

    def sweep_body(sweep, carry):
        last = sweep == SWEEPS - 1

        def s0(d):
            @pl.when(sweep == 0)
            def _():
                load_c(d).wait()

            def tile(v, carry):
                w_tile(d, v)
                return carry
            lax.fori_loop(jnp.where(sweep == 0, 0, NV - 1), NV, tile, 0)
            copy_a(d).start()

        def s1(d):
            copy_a(d).wait_recv()
            own = rows_at(d * dt + core * half, half)
            a_w[own, :] += r_a[rows_at(d * half, half), :]
            copy_x(d).start()

        def s2(d):
            @pl.when(d == 0)
            def _():
                take_sh()
                sw_acc[...] = jnp.zeros_like(sw_acc)
            copy_x(d).wait_recv()
            own = rows_at(d * quarter, quarter)
            fresh = w_f[own, :] * (a_w[mine(d), :] + r_x[own, :]) / sh_row[0:1, :]
            w_f[own, :] = fresh
            w_bf[mine(d), :] = fresh.astype(BF16)
            copy_g(d).start()
            copy_p(d).start()
            sw_acc[...] += jnp.sum(fresh.reshape(quarter // 8, 8, topics), axis=0)

            @pl.when(d == ND - 1)
            def _():
                send_sw()

        def s3(d):
            copy_g(d).wait_recv()
            copy_q(d).start()

        def s5(d):
            copy_p(d).wait_recv()
            copy_q(d).wait_recv()
            w_t[...] = w_bf[rows_at(d * dt, dt), :].T

            def tile(v):
                h_tile(d, v)

                @pl.when(jnp.logical_and(d == ND - 1, v < 2))
                def _():
                    copy_y(v).start()
            each(NV, tile)

        def stage(it, lag, body):
            @pl.when(jnp.logical_and(it >= lag, it < lag + ND))
            def _():
                body(it - lag)

        def w_step(it):
            stage(it, 0, s0)
            stage(it, 1, s1)
            stage(it, 3, s2)
            stage(it, 5, s5)
            stage(it, 4, s3)

        each(ND + 5, w_step)

        def w_sent(d):
            copy_a(d).wait_send()
            copy_x(d).wait_send()
            copy_g(d).wait_send()
            copy_p(d).wait_send()
            copy_q(d).wait_send()

        each(ND, w_sent)

        @pl.when(last)
        def _():
            def give(d):
                out_w(d).start()
                for step in range(1, cols):
                    copy_wo(d, step).start()
            each(ND, give)

        def t1(v):
            @pl.when(v == 0)
            def _():
                take_sw()
                sh_acc[...] = jnp.zeros_like(sh_acc)
            copy_y(v).wait_recv()
            for g in range(vt // LANES):
                at = pl.ds(pl.multiple_of(v * vt + g * LANES, LANES), LANES)
                fresh = h_f[:, at] * (a_h[own_k, at] + r_y[:, at]) / sw_col[...]
                h_f[:, at] = fresh
                h_bf[own_k, at] = fresh.astype(BF16)
                sh_acc[...] += fresh

            @pl.when(jnp.logical_not(last))
            def _():
                copy_z(v).start()

                @pl.when(v == NV - 1)
                def _():
                    send_sh()

            @pl.when(last)
            def _():
                out_h(v).start()
                copy_ho(v).start()

            @pl.when(v + 2 < NV)
            def _():
                copy_y(v + 2).start()

        def t3(v):
            copy_z(v).wait_recv()
            h_t[words_at(v), :] = h_bf[:, words_at(v)].T

            @pl.when(v < NV - 1)
            def _():
                each(ND, lambda d: w_tile(d, v))

        def h_step(it):
            @pl.when(it < NV)
            def _():
                t1(it)

            @pl.when(jnp.logical_and(it >= 1, jnp.logical_not(last)))
            def _():
                t3(it - 1)

        each(NV + 1, h_step)

        def h_sent(v):
            copy_y(v).wait_send()

            @pl.when(jnp.logical_not(last))
            def _():
                copy_z(v).wait_send()

        each(NV, h_sent)
        return carry

    lax.fori_loop(0, SWEEPS, sweep_body, 0)

    def finish_w(d):
        out_w(d).wait()
        for step in range(1, cols):
            copy_wo(d, step).wait()

    def finish_h(v):
        out_h(v).wait()
        copy_ho(v).wait()

    each(ND, finish_w)
    each(NV, finish_h)


def solution(mesh):
    rows, cols = mesh.shape["row"], mesh.shape["col"]
    n_dev = rows * cols

    def local(c_blk, w_loc, h_loc):
        docs, words = c_blk.shape
        topics = w_loc.shape[1]
        vmem = pltpu.VMEM
        dma = pltpu.SemaphoreType.DMA
        scratch = [
            vmem((docs, words), BF16),
            vmem((docs, topics), BF16),
            vmem((topics, docs // ND), BF16),
            vmem((topics, words), BF16),
            vmem((words, topics), BF16),
            vmem((docs // 4, topics), F32),
            vmem((topics // 2, words), F32),
            vmem((docs, topics), F32),
            vmem((topics, words), F32),
            vmem((docs // 2, topics), F32),
            vmem((docs // 4, topics), F32),
            vmem((topics // 2, words), F32),
            vmem((8, topics), F32),
            vmem((n_dev, 8, topics), F32),
            vmem((topics // 2, LANES), F32),
            vmem((topics // 2, LANES), F32),
            vmem((8, topics // 2), F32),
            vmem((n_dev, 8, topics // 2), F32),
            vmem((8, topics), F32),
            dma((2,)),
            dma((ND,)),
        ]
        scratch += [dma((ND,))] * 10
        scratch += [dma((NV,))] * 4
        scratch += [dma((n_dev - 1,))] * 4
        scratch += [dma((ND * (cols - 1),))] * 2
        scratch += [dma((NV,))] * 2
        scratch += [dma((ND,)), dma((NV,))]
        any_space = pl.BlockSpec(memory_space=pl.ANY)
        return pl.pallas_call(
            functools.partial(kernel, rows, cols),
            out_shape=(jax.ShapeDtypeStruct(w_loc.shape, F32), jax.ShapeDtypeStruct(h_loc.shape, F32)),
            in_specs=[any_space] * 3,
            out_specs=(any_space, any_space),
            scratch_shapes=scratch,
            compiler_params=pltpu.CompilerParams(
                collective_id=0, has_side_effects=True, vmem_limit_bytes=67_043_328),
            name="nmf",
        )(c_blk, w_loc, h_loc)

    spec_c = P(("part", "row"), "col")
    spec_w = P(("part", "row"), None)
    spec_h = P(None, ("part", "col"))
    return jax.shard_map(local, mesh=mesh, in_specs=(spec_c, spec_w, spec_h), out_specs=(spec_w, spec_h), check_vma=False)
```

```python
import functools

import jax
import jax.numpy as jnp
from jax import lax
from jax.experimental import pallas as pl
from jax.experimental.pallas import tpu as pltpu
from jax.sharding import PartitionSpec as P

SWEEPS = 4
EPS = 1e-6
ND = 8
NV = 8
LANES = 128
MESH = pl.DeviceIdType.MESH
F32 = jnp.float32
BF16 = jnp.bfloat16


def kernel(
    rows, cols, c_hbm, w_hbm, h_hbm, w_out, h_out,
    c_v, w_bf, w_t, h_bf, h_t, w_f, h_f, a_w, a_h, r_a, r_x, r_y,
    sw_acc, sw_slots, sw_col, sh_acc, sh_part, sh_slots, sh_row,
    load_sem, h_sem, c_sem,
    a_send, a_recv, x_send, x_recv, g_send, g_recv, p_send, p_recv, q_send, q_recv,
    y_send, y_recv, z_send, z_recv, sw_send, sw_recv, sh_send, sh_recv,
    wo_send, wo_recv, ho_send, ho_recv, ow_sem, oh_sem,
):
    docs, words = c_v.shape
    topics = w_bf.shape[1]
    dt, vt, kh = docs // ND, words // NV, topics // 2
    half, quarter = dt // 2, dt // 4
    n_dev = rows * cols
    y, i = lax.axis_index("row"), lax.axis_index("col")
    x, core = i // 2, i % 2
    me = y * cols + i
    partner = {"col": x * 2 + (1 - core)}
    across = {"col": (1 - x) * 2 + core}
    above = {"row": 1 - y}

    def peer(step):
        other = (me + step) % n_dev
        return {"row": other // cols, "col": other % cols}

    def rows_at(start, size):
        return pl.ds(pl.multiple_of(start, size), size)

    def remote(src, dst, send, recv, device):
        return pltpu.make_async_remote_copy(
            src_ref=src, dst_ref=dst, send_sem=send, recv_sem=recv, device_id=device, device_id_type=MESH)

    def mine(d):
        return rows_at(d * dt + core * half + x * quarter, quarter)

    def theirs(d):
        return rows_at(d * dt + core * half + (1 - x) * quarter, quarter)

    def copy_a(d):
        return remote(a_w.at[rows_at(d * dt + (1 - core) * half, half)], r_a.at[rows_at(d * half, half)],
                      a_send.at[d], a_recv.at[d], partner)

    def copy_x(d):
        return remote(a_w.at[theirs(d)], r_x.at[rows_at(d * quarter, quarter)], x_send.at[d], x_recv.at[d], across)

    def copy_g(d):
        return remote(w_bf.at[mine(d)], w_bf.at[mine(d)], g_send.at[d], g_recv.at[d], across)

    def copy_p(d):
        return remote(w_bf.at[mine(d)], w_bf.at[mine(d)], p_send.at[d], p_recv.at[d], partner)

    def copy_q(d):
        return remote(w_bf.at[theirs(d)], w_bf.at[theirs(d)], q_send.at[d], q_recv.at[d], partner)

    own_k, other_k = rows_at(y * kh, kh), rows_at((1 - y) * kh, kh)

    def words_at(v):
        return rows_at(v * vt, vt)

    def copy_y(v):
        return remote(a_h.at[v, other_k], r_y.at[v], y_send.at[v], y_recv.at[v], above)

    def copy_z(v):
        return remote(h_bf.at[v, own_k], h_bf.at[v, own_k], z_send.at[v], z_recv.at[v], above)

    def copy_sw(step):
        return remote(sw_acc, sw_slots.at[me], sw_send.at[step - 1], sw_recv.at[step - 1], peer(step))

    def copy_sh(step):
        return remote(sh_part, sh_slots.at[me], sh_send.at[step - 1], sh_recv.at[step - 1], peer(step))

    def copy_wo(d, step):
        k = d * (cols - 1) + step - 1
        return remote(w_f.at[rows_at(d * quarter, quarter)], w_out.at[mine(d)], wo_send.at[k], wo_recv.at[k],
                      {"col": (i + step) % cols})

    def copy_ho(v):
        return remote(h_f.at[v], h_out.at[own_k, words_at(v)], ho_send.at[v], ho_recv.at[v], above)

    def out_w(d):
        return pltpu.make_async_copy(w_f.at[rows_at(d * quarter, quarter)], w_out.at[mine(d)], ow_sem.at[d])

    def out_h(v):
        return pltpu.make_async_copy(h_f.at[v], h_out.at[own_k, words_at(v)], oh_sem.at[v])

    def load_c(d):
        return pltpu.make_async_copy(c_hbm.at[rows_at(d * dt, dt)], c_v.at[rows_at(d * dt, dt)], c_sem.at[d])

    def each(count, body):
        def step(n, carry):
            body(n)
            return carry
        lax.fori_loop(0, count, step, 0)

    def ratio(d, v):
        z = jnp.dot(w_bf[rows_at(d * dt, dt), :], h_bf[v], preferred_element_type=F32)
        return (c_v[rows_at(d * dt, dt), words_at(v)].astype(F32) / (z + EPS)).astype(BF16)

    def w_tile(d, v):
        part = jnp.dot(ratio(d, v), h_t[words_at(v), :], preferred_element_type=F32)
        held = a_w[rows_at(d * dt, dt), :]
        a_w[rows_at(d * dt, dt), :] = jnp.where(v == 0, 0.0, held) + part

    def h_tile(d, v):
        part = jnp.dot(w_t[...], ratio(d, v), preferred_element_type=F32)
        held = a_h[v]
        a_h[v] = jnp.where(d == 0, 0.0, held) + part

    def fold_lanes(block):
        total = block[:, :LANES]
        for g in range(1, block.shape[1] // LANES):
            total = total + block[:, g * LANES:(g + 1) * LANES]
        return total

    def send_sh():
        sh_part[...] = jnp.sum(sh_acc[...].T.reshape(LANES // 8, 8, kh), axis=0)
        sh_slots[me] = sh_part[...]
        for step in range(1, n_dev):
            copy_sh(step).start()

    def take_sh():
        for step in range(1, n_dev):
            copy_sh(step).wait()
        for r in range(rows):
            total = sh_slots[r * cols]
            for n in range(1, cols):
                total = total + sh_slots[r * cols + n]
            sh_row[:, r * kh:(r + 1) * kh] = jnp.broadcast_to(jnp.sum(total, axis=0, keepdims=True), (8, kh))

    def send_sw():
        sw_slots[me] = sw_acc[...]
        for step in range(1, n_dev):
            copy_sw(step).start()

    def take_sw():
        for step in range(1, n_dev):
            copy_sw(step).wait()
        total = sw_slots[0]
        for n in range(1, n_dev):
            total = total + sw_slots[n]
        total = jnp.sum(total, axis=0, keepdims=True)
        own = jnp.where(y == 0, total[:, :kh], total[:, kh:])
        sw_col[...] = jnp.broadcast_to(own, (LANES, kh)).T

    def load_h(v):
        return pltpu.make_async_copy(h_hbm.at[:, words_at(v)], a_h.at[v], h_sem.at[v])

    load_w = pltpu.make_async_copy(w_hbm, a_w, load_sem.at[0])
    each(NV, lambda v: load_h(v).start())
    load_w.start()
    for d in range(ND):
        load_c(d).start()
    barrier = pltpu.get_barrier_semaphore()
    for step in range(1, n_dev):
        pl.semaphore_signal(barrier, inc=1, device_id=peer(step), device_id_type=MESH)
    pl.semaphore_wait(barrier, n_dev - 1)

    sh_acc[...] = jnp.zeros_like(sh_acc)

    def start_h(v):
        load_h(v).wait()
        h_bf[v] = a_h[v].astype(BF16)
        own = a_h[v, own_k]
        h_f[v] = own
        sh_acc[...] += fold_lanes(own)
        h_t[words_at(v), :] = h_bf[v].T

    each(NV, start_h)
    send_sh()
    load_w.wait()

    def start_w(d):
        w_bf[rows_at(d * dt, dt), :] = a_w[rows_at(d * dt, dt), :].astype(BF16)
        w_f[rows_at(d * quarter, quarter), :] = a_w[mine(d), :]

    each(ND, start_w)

    def sweep_body(sweep, carry):
        last = sweep == SWEEPS - 1

        def s0(d):
            @pl.when(sweep == 0)
            def _():
                load_c(d).wait()

            def tile(v, carry):
                w_tile(d, v)
                return carry
            lax.fori_loop(jnp.where(sweep == 0, 0, NV - 1), NV, tile, 0)
            copy_a(d).start()

        def s1(d):
            copy_a(d).wait_recv()
            own = rows_at(d * dt + core * half, half)
            a_w[own, :] += r_a[rows_at(d * half, half), :]
            copy_x(d).start()

        def s2(d):
            @pl.when(d == 0)
            def _():
                take_sh()
                sw_acc[...] = jnp.zeros_like(sw_acc)
            copy_x(d).wait_recv()
            own = rows_at(d * quarter, quarter)
            fresh = w_f[own, :] * (a_w[mine(d), :] + r_x[own, :]) / sh_row[0:1, :]
            w_f[own, :] = fresh
            w_bf[mine(d), :] = fresh.astype(BF16)
            copy_g(d).start()
            copy_p(d).start()
            sw_acc[...] += jnp.sum(fresh.reshape(quarter // 8, 8, topics), axis=0)

            @pl.when(d == ND - 1)
            def _():
                send_sw()

        def s3(d):
            copy_g(d).wait_recv()
            copy_q(d).start()

        def s5(d):
            copy_p(d).wait_recv()
            copy_q(d).wait_recv()
            w_t[...] = w_bf[rows_at(d * dt, dt), :].T

            def tile(v):
                h_tile(d, v)

                @pl.when(jnp.logical_and(d == ND - 1, v < 2))
                def _():
                    copy_y(v).start()
            each(NV, tile)

        def stage(it, lag, body):
            @pl.when(jnp.logical_and(it >= lag, it < lag + ND))
            def _():
                body(it - lag)

        def w_step(it):
            stage(it, 0, s0)
            stage(it, 1, s1)
            stage(it, 3, s2)
            stage(it, 5, s5)
            stage(it, 4, s3)

        each(ND + 5, w_step)

        def w_sent(d):
            copy_a(d).wait_send()
            copy_x(d).wait_send()
            copy_g(d).wait_send()
            copy_p(d).wait_send()
            copy_q(d).wait_send()

        each(ND, w_sent)

        @pl.when(last)
        def _():
            def give(d):
                out_w(d).start()
                for step in range(1, cols):
                    copy_wo(d, step).start()
            each(ND, give)

        def t1(v):
            @pl.when(v == 0)
            def _():
                take_sw()
                sh_acc[...] = jnp.zeros_like(sh_acc)
            copy_y(v).wait_recv()
            for g in range(vt // LANES):
                at = slice(g * LANES, (g + 1) * LANES)
                fresh = h_f[v, :, at] * (a_h[v, own_k, at] + r_y[v, :, at]) / sw_col[...]
                h_f[v, :, at] = fresh
                h_bf[v, own_k, at] = fresh.astype(BF16)
                sh_acc[...] += fresh

            @pl.when(jnp.logical_not(last))
            def _():
                copy_z(v).start()

                @pl.when(v == NV - 1)
                def _():
                    send_sh()

            @pl.when(last)
            def _():
                out_h(v).start()
                copy_ho(v).start()

            @pl.when(v + 2 < NV)
            def _():
                copy_y(v + 2).start()

        def t3(v):
            copy_z(v).wait_recv()
            h_t[words_at(v), :] = h_bf[v].T

            @pl.when(v < NV - 1)
            def _():
                each(ND, lambda d: w_tile(d, v))

        def h_step(it):
            @pl.when(it < NV)
            def _():
                t1(it)

            @pl.when(jnp.logical_and(it >= 1, jnp.logical_not(last)))
            def _():
                t3(it - 1)

        each(NV + 1, h_step)

        def h_sent(v):
            copy_y(v).wait_send()

            @pl.when(jnp.logical_not(last))
            def _():
                copy_z(v).wait_send()

        each(NV, h_sent)
        return carry

    lax.fori_loop(0, SWEEPS, sweep_body, 0)

    def finish_w(d):
        out_w(d).wait()
        for step in range(1, cols):
            copy_wo(d, step).wait()

    def finish_h(v):
        out_h(v).wait()
        copy_ho(v).wait()

    each(ND, finish_w)
    each(NV, finish_h)


def solution(mesh):
    rows, cols = mesh.shape["row"], mesh.shape["col"]
    n_dev = rows * cols

    def local(c_blk, w_loc, h_loc):
        docs, words = c_blk.shape
        topics = w_loc.shape[1]
        vmem = pltpu.VMEM
        dma = pltpu.SemaphoreType.DMA
        scratch = [
            vmem((docs, words), BF16),
            vmem((docs, topics), BF16),
            vmem((topics, docs // ND), BF16),
            vmem((NV, topics, words // NV), BF16),
            vmem((words, topics), BF16),
            vmem((docs // 4, topics), F32),
            vmem((NV, topics // 2, words // NV), F32),
            vmem((docs, topics), F32),
            vmem((NV, topics, words // NV), F32),
            vmem((docs // 2, topics), F32),
            vmem((docs // 4, topics), F32),
            vmem((NV, topics // 2, words // NV), F32),
            vmem((8, topics), F32),
            vmem((n_dev, 8, topics), F32),
            vmem((topics // 2, LANES), F32),
            vmem((topics // 2, LANES), F32),
            vmem((8, topics // 2), F32),
            vmem((n_dev, 8, topics // 2), F32),
            vmem((8, topics), F32),
            dma((1,)),
            dma((NV,)),
            dma((ND,)),
        ]
        scratch += [dma((ND,))] * 10
        scratch += [dma((NV,))] * 4
        scratch += [dma((n_dev - 1,))] * 4
        scratch += [dma((ND * (cols - 1),))] * 2
        scratch += [dma((NV,))] * 2
        scratch += [dma((ND,)), dma((NV,))]
        any_space = pl.BlockSpec(memory_space=pl.ANY)
        return pl.pallas_call(
            functools.partial(kernel, rows, cols),
            out_shape=(jax.ShapeDtypeStruct(w_loc.shape, F32), jax.ShapeDtypeStruct(h_loc.shape, F32)),
            in_specs=[any_space] * 3,
            out_specs=(any_space, any_space),
            scratch_shapes=scratch,
            compiler_params=pltpu.CompilerParams(
                collective_id=0, has_side_effects=True, vmem_limit_bytes=67_043_328),
            name="nmf",
        )(c_blk, w_loc, h_loc)

    spec_c = P(("part", "row"), "col")
    spec_w = P(("part", "row"), None)
    spec_h = P(None, ("part", "col"))
    return jax.shard_map(local, mesh=mesh, in_specs=(spec_c, spec_w, spec_h), out_specs=(spec_w, spec_h), check_vma=False)
```

```python
import functools

import jax
import jax.numpy as jnp
from jax import lax
from jax.experimental import pallas as pl
from jax.experimental.pallas import tpu as pltpu
from jax.sharding import PartitionSpec as P

SWEEPS = 4
EPS = 1e-6
ND = 8
NV = 8
GROUP = 4
LANES = 128
MESH = pl.DeviceIdType.MESH
F32 = jnp.float32
BF16 = jnp.bfloat16


def kernel(
    rows, cols, c_hbm, w_hbm, h_hbm, w_out, h_out,
    c_v, w_bf, w_t, h_bf, h_t, w_f, h_f, a_w, a_h, r_a, r_x, r_y,
    sw_acc, sw_slots, sw_col, sh_acc, sh_part, sh_slots, sh_row,
    load_sem, h_sem, c_sem,
    a_send, a_recv, x_send, x_recv, g_send, g_recv, p_send, p_recv, q_send, q_recv,
    y_send, y_recv, z_send, z_recv, sw_send, sw_recv, sh_send, sh_recv,
    wo_send, wo_recv, ho_send, ho_recv, ow_sem, oh_sem,
):
    docs, words = c_v.shape
    topics = w_bf.shape[1]
    dt, vt, kh = docs // ND, words // NV, topics // 2
    half, quarter = dt // 2, dt // 4
    n_dev = rows * cols
    y, i = lax.axis_index("row"), lax.axis_index("col")
    x, core = i // 2, i % 2
    me = y * cols + i
    partner = {"col": x * 2 + (1 - core)}
    across = {"col": (1 - x) * 2 + core}
    above = {"row": 1 - y}

    def peer(step):
        other = (me + step) % n_dev
        return {"row": other // cols, "col": other % cols}

    def rows_at(start, size):
        return pl.ds(pl.multiple_of(start, size), size)

    def remote(src, dst, send, recv, device):
        return pltpu.make_async_remote_copy(
            src_ref=src, dst_ref=dst, send_sem=send, recv_sem=recv, device_id=device, device_id_type=MESH)

    def mine(d):
        return rows_at(d * dt + core * half + x * quarter, quarter)

    def theirs(d):
        return rows_at(d * dt + core * half + (1 - x) * quarter, quarter)

    def copy_a(d):
        return remote(a_w.at[rows_at(d * dt + (1 - core) * half, half)], r_a.at[rows_at(d * half, half)],
                      a_send.at[d], a_recv.at[d], partner)

    def copy_x(d):
        return remote(a_w.at[theirs(d)], r_x.at[rows_at(d * quarter, quarter)], x_send.at[d], x_recv.at[d], across)

    def copy_g(d):
        return remote(w_bf.at[mine(d)], w_bf.at[mine(d)], g_send.at[d], g_recv.at[d], across)

    def copy_p(d):
        return remote(w_bf.at[mine(d)], w_bf.at[mine(d)], p_send.at[d], p_recv.at[d], partner)

    def copy_q(d):
        return remote(w_bf.at[theirs(d)], w_bf.at[theirs(d)], q_send.at[d], q_recv.at[d], partner)

    own_k, other_k = rows_at(y * kh, kh), rows_at((1 - y) * kh, kh)

    def words_at(v):
        return rows_at(v * vt, vt)

    def copy_y(v):
        return remote(a_h.at[v, other_k], r_y.at[v], y_send.at[v], y_recv.at[v], above)

    def copy_z(v):
        return remote(h_bf.at[v, own_k], h_bf.at[v, own_k], z_send.at[v], z_recv.at[v], above)

    def copy_sw(step):
        return remote(sw_acc, sw_slots.at[me], sw_send.at[step - 1], sw_recv.at[step - 1], peer(step))

    def copy_sh(step):
        return remote(sh_part, sh_slots.at[me], sh_send.at[step - 1], sh_recv.at[step - 1], peer(step))

    def copy_wo(d, step):
        k = d * (cols - 1) + step - 1
        return remote(w_f.at[rows_at(d * quarter, quarter)], w_out.at[mine(d)], wo_send.at[k], wo_recv.at[k],
                      {"col": (i + step) % cols})

    def copy_ho(v):
        return remote(h_f.at[v], h_out.at[own_k, words_at(v)], ho_send.at[v], ho_recv.at[v], above)

    def out_w(d):
        return pltpu.make_async_copy(w_f.at[rows_at(d * quarter, quarter)], w_out.at[mine(d)], ow_sem.at[d])

    def out_h(v):
        return pltpu.make_async_copy(h_f.at[v], h_out.at[own_k, words_at(v)], oh_sem.at[v])

    def load_c(d):
        return pltpu.make_async_copy(c_hbm.at[rows_at(d * dt, dt)], c_v.at[rows_at(d * dt, dt)], c_sem.at[d])

    def each(count, body):
        def step(n, carry):
            body(n)
            return carry
        lax.fori_loop(0, count, step, 0)

    def ratio(d, v):
        z = jnp.dot(w_bf[rows_at(d * dt, dt), :], h_bf[v], preferred_element_type=F32)
        return (c_v[rows_at(d * dt, dt), words_at(v)].astype(F32) / (z + EPS)).astype(BF16)

    def w_tile(d, v):
        part = jnp.dot(ratio(d, v), h_t[words_at(v), :], preferred_element_type=F32)
        held = a_w[rows_at(d * dt, dt), :]
        a_w[rows_at(d * dt, dt), :] = jnp.where(v == 0, 0.0, held) + part

    def h_tile(d, v):
        part = jnp.dot(w_t[...], ratio(d, v), preferred_element_type=F32)
        held = a_h[v]
        a_h[v] = jnp.where(d == 0, 0.0, held) + part

    def fold_lanes(block):
        total = block[:, :LANES]
        for g in range(1, block.shape[1] // LANES):
            total = total + block[:, g * LANES:(g + 1) * LANES]
        return total

    def send_sh():
        sh_part[...] = jnp.sum(sh_acc[...].T.reshape(LANES // 8, 8, kh), axis=0)
        sh_slots[me] = sh_part[...]
        for step in range(1, n_dev):
            copy_sh(step).start()

    def take_sh():
        for step in range(1, n_dev):
            copy_sh(step).wait()
        for r in range(rows):
            total = sh_slots[r * cols]
            for n in range(1, cols):
                total = total + sh_slots[r * cols + n]
            sh_row[:, r * kh:(r + 1) * kh] = jnp.broadcast_to(jnp.sum(total, axis=0, keepdims=True), (8, kh))

    def send_sw():
        sw_slots[me] = sw_acc[...]
        for step in range(1, n_dev):
            copy_sw(step).start()

    def take_sw():
        for step in range(1, n_dev):
            copy_sw(step).wait()
        total = sw_slots[0]
        for n in range(1, n_dev):
            total = total + sw_slots[n]
        total = jnp.sum(total, axis=0, keepdims=True)
        own = jnp.where(y == 0, total[:, :kh], total[:, kh:])
        sw_col[...] = jnp.broadcast_to(own, (LANES, kh)).T

    def load_h(v):
        return pltpu.make_async_copy(h_hbm.at[:, words_at(v)], a_h.at[v], h_sem.at[v])

    load_w = pltpu.make_async_copy(w_hbm, a_w, load_sem.at[0])
    each(NV, lambda v: load_h(v).start())
    load_w.start()
    for d in range(ND):
        load_c(d).start()
    barrier = pltpu.get_barrier_semaphore()
    for step in range(1, n_dev):
        pl.semaphore_signal(barrier, inc=1, device_id=peer(step), device_id_type=MESH)
    pl.semaphore_wait(barrier, n_dev - 1)

    sh_acc[...] = jnp.zeros_like(sh_acc)

    def start_h(v):
        load_h(v).wait()
        h_bf[v] = a_h[v].astype(BF16)
        own = a_h[v, own_k]
        h_f[v] = own
        sh_acc[...] += fold_lanes(own)
        h_t[words_at(v), :] = h_bf[v].T

    each(NV, start_h)
    send_sh()
    load_w.wait()

    def start_w(d):
        w_bf[rows_at(d * dt, dt), :] = a_w[rows_at(d * dt, dt), :].astype(BF16)
        w_f[rows_at(d * quarter, quarter), :] = a_w[mine(d), :]

    each(ND, start_w)

    def sweep_body(sweep, carry):
        last = sweep == SWEEPS - 1

        def s0(d):
            @pl.when(sweep == 0)
            def _():
                load_c(d).wait()

            @pl.when(sweep == 0)
            def _():
                def group(n):
                    for k in range(GROUP):
                        w_tile(d, n * GROUP + k)
                each(NV // GROUP, group)

            @pl.when(sweep > 0)
            def _():
                w_tile(d, NV - 1)
            copy_a(d).start()

        def s1(d):
            copy_a(d).wait_recv()
            own = rows_at(d * dt + core * half, half)
            a_w[own, :] += r_a[rows_at(d * half, half), :]
            copy_x(d).start()

        def s2(d):
            @pl.when(d == 0)
            def _():
                take_sh()
                sw_acc[...] = jnp.zeros_like(sw_acc)
            copy_x(d).wait_recv()
            own = rows_at(d * quarter, quarter)
            fresh = w_f[own, :] * (a_w[mine(d), :] + r_x[own, :]) / sh_row[0:1, :]
            w_f[own, :] = fresh
            w_bf[mine(d), :] = fresh.astype(BF16)
            copy_g(d).start()
            copy_p(d).start()
            sw_acc[...] += jnp.sum(fresh.reshape(quarter // 8, 8, topics), axis=0)

            @pl.when(d == ND - 1)
            def _():
                send_sw()

        def s3(d):
            copy_g(d).wait_recv()
            copy_q(d).start()

        def s5(d):
            copy_p(d).wait_recv()
            copy_q(d).wait_recv()
            w_t[...] = w_bf[rows_at(d * dt, dt), :].T

            def group(n):
                for k in range(GROUP):
                    h_tile(d, n * GROUP + k)

                @pl.when(jnp.logical_and(d == ND - 1, n == 0))
                def _():
                    copy_y(0).start()
                    copy_y(1).start()
            each(NV // GROUP, group)

        def stage(it, lag, body):
            @pl.when(jnp.logical_and(it >= lag, it < lag + ND))
            def _():
                body(it - lag)

        def w_step(it):
            stage(it, 0, s0)
            stage(it, 1, s1)
            stage(it, 3, s2)
            stage(it, 5, s5)
            stage(it, 4, s3)

        each(ND + 5, w_step)

        def w_sent(d):
            copy_a(d).wait_send()
            copy_x(d).wait_send()
            copy_g(d).wait_send()
            copy_p(d).wait_send()
            copy_q(d).wait_send()

        each(ND, w_sent)

        @pl.when(last)
        def _():
            def give(d):
                out_w(d).start()
                for step in range(1, cols):
                    copy_wo(d, step).start()
            each(ND, give)

        def t1(v):
            @pl.when(v == 0)
            def _():
                take_sw()
                sh_acc[...] = jnp.zeros_like(sh_acc)
            copy_y(v).wait_recv()
            for g in range(vt // LANES):
                at = slice(g * LANES, (g + 1) * LANES)
                fresh = h_f[v, :, at] * (a_h[v, own_k, at] + r_y[v, :, at]) / sw_col[...]
                h_f[v, :, at] = fresh
                h_bf[v, own_k, at] = fresh.astype(BF16)
                sh_acc[...] += fresh

            @pl.when(jnp.logical_not(last))
            def _():
                copy_z(v).start()

                @pl.when(v == NV - 1)
                def _():
                    send_sh()

            @pl.when(last)
            def _():
                out_h(v).start()
                copy_ho(v).start()

            @pl.when(v + 2 < NV)
            def _():
                copy_y(v + 2).start()

        def t3(v):
            copy_z(v).wait_recv()
            h_t[words_at(v), :] = h_bf[v].T

            @pl.when(v < NV - 1)
            def _():
                def group(n):
                    for k in range(GROUP):
                        w_tile(n * GROUP + k, v)
                each(ND // GROUP, group)

        def h_step(it):
            @pl.when(it < NV)
            def _():
                t1(it)

            @pl.when(jnp.logical_and(it >= 1, jnp.logical_not(last)))
            def _():
                t3(it - 1)

        each(NV + 1, h_step)

        def h_sent(v):
            copy_y(v).wait_send()

            @pl.when(jnp.logical_not(last))
            def _():
                copy_z(v).wait_send()

        each(NV, h_sent)
        return carry

    lax.fori_loop(0, SWEEPS, sweep_body, 0)

    def finish_w(d):
        out_w(d).wait()
        for step in range(1, cols):
            copy_wo(d, step).wait()

    def finish_h(v):
        out_h(v).wait()
        copy_ho(v).wait()

    each(ND, finish_w)
    each(NV, finish_h)


def solution(mesh):
    rows, cols = mesh.shape["row"], mesh.shape["col"]
    n_dev = rows * cols

    def local(c_blk, w_loc, h_loc):
        docs, words = c_blk.shape
        topics = w_loc.shape[1]
        vmem = pltpu.VMEM
        dma = pltpu.SemaphoreType.DMA
        scratch = [
            vmem((docs, words), BF16),
            vmem((docs, topics), BF16),
            vmem((topics, docs // ND), BF16),
            vmem((NV, topics, words // NV), BF16),
            vmem((words, topics), BF16),
            vmem((docs // 4, topics), F32),
            vmem((NV, topics // 2, words // NV), F32),
            vmem((docs, topics), F32),
            vmem((NV, topics, words // NV), F32),
            vmem((docs // 2, topics), F32),
            vmem((docs // 4, topics), F32),
            vmem((NV, topics // 2, words // NV), F32),
            vmem((8, topics), F32),
            vmem((n_dev, 8, topics), F32),
            vmem((topics // 2, LANES), F32),
            vmem((topics // 2, LANES), F32),
            vmem((8, topics // 2), F32),
            vmem((n_dev, 8, topics // 2), F32),
            vmem((8, topics), F32),
            dma((1,)),
            dma((NV,)),
            dma((ND,)),
        ]
        scratch += [dma((ND,))] * 10
        scratch += [dma((NV,))] * 4
        scratch += [dma((n_dev - 1,))] * 4
        scratch += [dma((ND * (cols - 1),))] * 2
        scratch += [dma((NV,))] * 2
        scratch += [dma((ND,)), dma((NV,))]
        any_space = pl.BlockSpec(memory_space=pl.ANY)
        return pl.pallas_call(
            functools.partial(kernel, rows, cols),
            out_shape=(jax.ShapeDtypeStruct(w_loc.shape, F32), jax.ShapeDtypeStruct(h_loc.shape, F32)),
            in_specs=[any_space] * 3,
            out_specs=(any_space, any_space),
            scratch_shapes=scratch,
            compiler_params=pltpu.CompilerParams(
                collective_id=0, has_side_effects=True, vmem_limit_bytes=67_043_328),
            name="nmf",
        )(c_blk, w_loc, h_loc)

    spec_c = P(("part", "row"), "col")
    spec_w = P(("part", "row"), None)
    spec_h = P(None, ("part", "col"))
    return jax.shard_map(local, mesh=mesh, in_specs=(spec_c, spec_w, spec_h), out_specs=(spec_w, spec_h), check_vma=False)
```

```python
import functools

import jax
import jax.numpy as jnp
from jax import lax
from jax.experimental import pallas as pl
from jax.experimental.pallas import tpu as pltpu
from jax.sharding import PartitionSpec as P

SWEEPS = 4
EPS = 1e-6
ND = 8
NV = 8
GROUP = 4
LAG1, LAG2, LAG3, LAG5 = 2, 4, 5, 6
LANES = 128
MESH = pl.DeviceIdType.MESH
F32 = jnp.float32
BF16 = jnp.bfloat16


def kernel(
    rows, cols, c_hbm, w_hbm, h_hbm, w_out, h_out,
    c_v, w_bf, w_t, h_bf, h_t, w_f, h_f, a_w, a_h, r_a, r_x, r_y,
    sw_acc, sw_slots, sw_col, sh_acc, sh_part, sh_slots, sh_row,
    load_sem, h_sem, c_sem,
    a_send, a_recv, x_send, x_recv, g_send, g_recv, p_send, p_recv, q_send, q_recv,
    y_send, y_recv, z_send, z_recv, sw_send, sw_recv, sh_send, sh_recv,
    wo_send, wo_recv, ho_send, ho_recv, ow_sem, oh_sem,
):
    docs, words = c_v.shape
    topics = w_bf.shape[1]
    dt, vt, kh = docs // ND, words // NV, topics // 2
    half, quarter = dt // 2, dt // 4
    n_dev = rows * cols
    y, i = lax.axis_index("row"), lax.axis_index("col")
    x, core = i // 2, i % 2
    me = y * cols + i
    partner = {"col": x * 2 + (1 - core)}
    across = {"col": (1 - x) * 2 + core}
    above = {"row": 1 - y}

    def peer(step):
        other = (me + step) % n_dev
        return {"row": other // cols, "col": other % cols}

    def rows_at(start, size):
        return pl.ds(pl.multiple_of(start, size), size)

    def remote(src, dst, send, recv, device):
        return pltpu.make_async_remote_copy(
            src_ref=src, dst_ref=dst, send_sem=send, recv_sem=recv, device_id=device, device_id_type=MESH)

    def mine(d):
        return rows_at(d * dt + core * half + x * quarter, quarter)

    def theirs(d):
        return rows_at(d * dt + core * half + (1 - x) * quarter, quarter)

    def copy_a(d):
        return remote(a_w.at[rows_at(d * dt + (1 - core) * half, half)], r_a.at[rows_at(d * half, half)],
                      a_send.at[d], a_recv.at[d], partner)

    def copy_x(d):
        return remote(a_w.at[theirs(d)], r_x.at[rows_at(d * quarter, quarter)], x_send.at[d], x_recv.at[d], across)

    def copy_g(d):
        return remote(w_bf.at[mine(d)], w_bf.at[mine(d)], g_send.at[d], g_recv.at[d], across)

    def copy_p(d):
        return remote(w_bf.at[mine(d)], w_bf.at[mine(d)], p_send.at[d], p_recv.at[d], partner)

    def copy_q(d):
        return remote(w_bf.at[theirs(d)], w_bf.at[theirs(d)], q_send.at[d], q_recv.at[d], partner)

    own_k, other_k = rows_at(y * kh, kh), rows_at((1 - y) * kh, kh)

    def words_at(v):
        return rows_at(v * vt, vt)

    def copy_y(v):
        return remote(a_h.at[v, other_k], r_y.at[v], y_send.at[v], y_recv.at[v], above)

    def copy_z(v):
        return remote(h_bf.at[v, own_k], h_bf.at[v, own_k], z_send.at[v], z_recv.at[v], above)

    def copy_sw(step):
        return remote(sw_acc, sw_slots.at[me], sw_send.at[step - 1], sw_recv.at[step - 1], peer(step))

    def copy_sh(step):
        return remote(sh_part, sh_slots.at[me], sh_send.at[step - 1], sh_recv.at[step - 1], peer(step))

    def copy_wo(d, step):
        k = d * (cols - 1) + step - 1
        return remote(w_f.at[rows_at(d * quarter, quarter)], w_out.at[mine(d)], wo_send.at[k], wo_recv.at[k],
                      {"col": (i + step) % cols})

    def copy_ho(v):
        return remote(h_f.at[v], h_out.at[own_k, words_at(v)], ho_send.at[v], ho_recv.at[v], above)

    def out_w(d):
        return pltpu.make_async_copy(w_f.at[rows_at(d * quarter, quarter)], w_out.at[mine(d)], ow_sem.at[d])

    def out_h(v):
        return pltpu.make_async_copy(h_f.at[v], h_out.at[own_k, words_at(v)], oh_sem.at[v])

    def load_c(d):
        return pltpu.make_async_copy(c_hbm.at[rows_at(d * dt, dt)], c_v.at[rows_at(d * dt, dt)], c_sem.at[d])

    def each(count, body):
        def step(n, carry):
            body(n)
            return carry
        lax.fori_loop(0, count, step, 0)

    def ratio(d, v):
        z = jnp.dot(w_bf[rows_at(d * dt, dt), :], h_bf[v], preferred_element_type=F32)
        return (c_v[rows_at(d * dt, dt), words_at(v)].astype(F32) / (z + EPS)).astype(BF16)

    def w_tile(d, v):
        part = jnp.dot(ratio(d, v), h_t[words_at(v), :], preferred_element_type=F32)
        held = a_w[rows_at(d * dt, dt), :]
        a_w[rows_at(d * dt, dt), :] = jnp.where(v == 0, 0.0, held) + part

    def h_tile(d, v):
        part = jnp.dot(w_t[...], ratio(d, v), preferred_element_type=F32)
        held = a_h[v]
        a_h[v] = jnp.where(d == 0, 0.0, held) + part

    def fold_lanes(block):
        total = block[:, :LANES]
        for g in range(1, block.shape[1] // LANES):
            total = total + block[:, g * LANES:(g + 1) * LANES]
        return total

    def send_sh():
        sh_part[...] = jnp.sum(sh_acc[...].T.reshape(LANES // 8, 8, kh), axis=0)
        sh_slots[me] = sh_part[...]
        for step in range(1, n_dev):
            copy_sh(step).start()

    def take_sh():
        for step in range(1, n_dev):
            copy_sh(step).wait()
        for r in range(rows):
            total = sh_slots[r * cols]
            for n in range(1, cols):
                total = total + sh_slots[r * cols + n]
            sh_row[:, r * kh:(r + 1) * kh] = jnp.broadcast_to(jnp.sum(total, axis=0, keepdims=True), (8, kh))

    def send_sw():
        sw_slots[me] = sw_acc[...]
        for step in range(1, n_dev):
            copy_sw(step).start()

    def take_sw():
        for step in range(1, n_dev):
            copy_sw(step).wait()
        total = sw_slots[0]
        for n in range(1, n_dev):
            total = total + sw_slots[n]
        total = jnp.sum(total, axis=0, keepdims=True)
        own = jnp.where(y == 0, total[:, :kh], total[:, kh:])
        sw_col[...] = jnp.broadcast_to(own, (LANES, kh)).T

    def load_h(v):
        return pltpu.make_async_copy(h_hbm.at[:, words_at(v)], a_h.at[v], h_sem.at[v])

    load_w = pltpu.make_async_copy(w_hbm, a_w, load_sem.at[0])
    each(NV, lambda v: load_h(v).start())
    load_w.start()
    for d in range(ND):
        load_c(d).start()
    barrier = pltpu.get_barrier_semaphore()
    for step in range(1, n_dev):
        pl.semaphore_signal(barrier, inc=1, device_id=peer(step), device_id_type=MESH)
    pl.semaphore_wait(barrier, n_dev - 1)

    sh_acc[...] = jnp.zeros_like(sh_acc)

    def start_h(v):
        load_h(v).wait()
        h_bf[v] = a_h[v].astype(BF16)
        own = a_h[v, own_k]
        h_f[v] = own
        sh_acc[...] += fold_lanes(own)
        h_t[words_at(v), :] = h_bf[v].T

    each(NV, start_h)
    send_sh()
    load_w.wait()

    def start_w(d):
        w_bf[rows_at(d * dt, dt), :] = a_w[rows_at(d * dt, dt), :].astype(BF16)
        w_f[rows_at(d * quarter, quarter), :] = a_w[mine(d), :]

    each(ND, start_w)

    def sweep_body(sweep, carry):
        last = sweep == SWEEPS - 1

        def s0(d):
            @pl.when(sweep == 0)
            def _():
                load_c(d).wait()

            @pl.when(sweep == 0)
            def _():
                def group(n):
                    for k in range(GROUP):
                        w_tile(d, n * GROUP + k)
                each(NV // GROUP, group)

            @pl.when(sweep > 0)
            def _():
                w_tile(d, NV - 1)
            copy_a(d).start()

        def s1(d):
            copy_a(d).wait_recv()
            own = rows_at(d * dt + core * half, half)
            a_w[own, :] += r_a[rows_at(d * half, half), :]
            copy_x(d).start()

        def s2(d):
            @pl.when(d == 0)
            def _():
                take_sh()
                sw_acc[...] = jnp.zeros_like(sw_acc)
            copy_x(d).wait_recv()
            own = rows_at(d * quarter, quarter)
            fresh = w_f[own, :] * (a_w[mine(d), :] + r_x[own, :]) / sh_row[0:1, :]
            w_f[own, :] = fresh
            w_bf[mine(d), :] = fresh.astype(BF16)
            copy_g(d).start()
            copy_p(d).start()
            sw_acc[...] += jnp.sum(fresh.reshape(quarter // 8, 8, topics), axis=0)

            @pl.when(d == ND - 1)
            def _():
                send_sw()

        def s3(d):
            copy_g(d).wait_recv()
            copy_q(d).start()

        def s5(d):
            copy_p(d).wait_recv()
            copy_q(d).wait_recv()
            w_t[...] = w_bf[rows_at(d * dt, dt), :].T

            def group(n):
                for k in range(GROUP):
                    h_tile(d, n * GROUP + k)

                @pl.when(jnp.logical_and(d == ND - 1, n == 0))
                def _():
                    copy_y(0).start()
                    copy_y(1).start()
            each(NV // GROUP, group)

        def stage(it, lag, body):
            @pl.when(jnp.logical_and(it >= lag, it < lag + ND))
            def _():
                body(it - lag)

        def w_step(it):
            for lag, body in ((LAG2, s2), (LAG1, s1), (0, s0), (LAG3, s3), (LAG5, s5)):
                stage(it, lag, body)

        each(ND + LAG5, w_step)

        def w_sent(d):
            copy_a(d).wait_send()
            copy_x(d).wait_send()
            copy_g(d).wait_send()
            copy_p(d).wait_send()
            copy_q(d).wait_send()

        each(ND, w_sent)

        @pl.when(last)
        def _():
            def give(d):
                out_w(d).start()
                for step in range(1, cols):
                    copy_wo(d, step).start()
            each(ND, give)

        def t1(v):
            @pl.when(v == 0)
            def _():
                take_sw()
                sh_acc[...] = jnp.zeros_like(sh_acc)
            copy_y(v).wait_recv()
            for g in range(vt // LANES):
                at = slice(g * LANES, (g + 1) * LANES)
                fresh = h_f[v, :, at] * (a_h[v, own_k, at] + r_y[v, :, at]) / sw_col[...]
                h_f[v, :, at] = fresh
                h_bf[v, own_k, at] = fresh.astype(BF16)
                sh_acc[...] += fresh

            @pl.when(jnp.logical_not(last))
            def _():
                copy_z(v).start()

                @pl.when(v == NV - 1)
                def _():
                    send_sh()

            @pl.when(last)
            def _():
                out_h(v).start()
                copy_ho(v).start()

            @pl.when(v + 2 < NV)
            def _():
                copy_y(v + 2).start()

        def t3(v):
            copy_z(v).wait_recv()
            h_t[words_at(v), :] = h_bf[v].T

            @pl.when(v < NV - 1)
            def _():
                def group(n):
                    for k in range(GROUP):
                        w_tile(n * GROUP + k, v)
                each(ND // GROUP, group)

        def h_step(it):
            @pl.when(it < NV)
            def _():
                t1(it)

            @pl.when(jnp.logical_and(it >= 1, jnp.logical_not(last)))
            def _():
                t3(it - 1)

        each(NV + 1, h_step)

        def h_sent(v):
            copy_y(v).wait_send()

            @pl.when(jnp.logical_not(last))
            def _():
                copy_z(v).wait_send()

        each(NV, h_sent)
        return carry

    lax.fori_loop(0, SWEEPS, sweep_body, 0)

    def finish_w(d):
        out_w(d).wait()
        for step in range(1, cols):
            copy_wo(d, step).wait()

    def finish_h(v):
        out_h(v).wait()
        copy_ho(v).wait()

    each(ND, finish_w)
    each(NV, finish_h)


def solution(mesh):
    rows, cols = mesh.shape["row"], mesh.shape["col"]
    n_dev = rows * cols

    def local(c_blk, w_loc, h_loc):
        docs, words = c_blk.shape
        topics = w_loc.shape[1]
        vmem = pltpu.VMEM
        dma = pltpu.SemaphoreType.DMA
        scratch = [
            vmem((docs, words), BF16),
            vmem((docs, topics), BF16),
            vmem((topics, docs // ND), BF16),
            vmem((NV, topics, words // NV), BF16),
            vmem((words, topics), BF16),
            vmem((docs // 4, topics), F32),
            vmem((NV, topics // 2, words // NV), F32),
            vmem((docs, topics), F32),
            vmem((NV, topics, words // NV), F32),
            vmem((docs // 2, topics), F32),
            vmem((docs // 4, topics), F32),
            vmem((NV, topics // 2, words // NV), F32),
            vmem((8, topics), F32),
            vmem((n_dev, 8, topics), F32),
            vmem((topics // 2, LANES), F32),
            vmem((topics // 2, LANES), F32),
            vmem((8, topics // 2), F32),
            vmem((n_dev, 8, topics // 2), F32),
            vmem((8, topics), F32),
            dma((1,)),
            dma((NV,)),
            dma((ND,)),
        ]
        scratch += [dma((ND,))] * 10
        scratch += [dma((NV,))] * 4
        scratch += [dma((n_dev - 1,))] * 4
        scratch += [dma((ND * (cols - 1),))] * 2
        scratch += [dma((NV,))] * 2
        scratch += [dma((ND,)), dma((NV,))]
        any_space = pl.BlockSpec(memory_space=pl.ANY)
        return pl.pallas_call(
            functools.partial(kernel, rows, cols),
            out_shape=(jax.ShapeDtypeStruct(w_loc.shape, F32), jax.ShapeDtypeStruct(h_loc.shape, F32)),
            in_specs=[any_space] * 3,
            out_specs=(any_space, any_space),
            scratch_shapes=scratch,
            compiler_params=pltpu.CompilerParams(
                collective_id=0, has_side_effects=True, vmem_limit_bytes=67_043_328),
            name="nmf",
        )(c_blk, w_loc, h_loc)

    spec_c = P(("part", "row"), "col")
    spec_w = P(("part", "row"), None)
    spec_h = P(None, ("part", "col"))
    return jax.shard_map(local, mesh=mesh, in_specs=(spec_c, spec_w, spec_h), out_specs=(spec_w, spec_h), check_vma=False)
```

```python
import functools

import jax
import jax.numpy as jnp
from jax import lax
from jax.experimental import pallas as pl
from jax.experimental.pallas import tpu as pltpu
from jax.sharding import PartitionSpec as P

SWEEPS = 4
EPS = 1e-6
ND = 8
NV = 8
GROUP = 4
LAG1, LAG2, LAG3, LAG5 = 2, 4, 5, 6
LANES = 128
MESH = pl.DeviceIdType.MESH
F32 = jnp.float32
BF16 = jnp.bfloat16


def kernel(
    rows, cols, c_hbm, w_hbm, h_hbm, w_out, h_out,
    c_v, w_bf, w_t, h_bf, h_t, w_f, h_f, a_w, a_h, r_a, r_x, r_y,
    sw_acc, sw_slots, sw_col, sh_acc, sh_part, sh_slots, sh_row,
    w_sem, h_sem, c_sem,
    a_send, a_recv, x_send, x_recv, g_send, g_recv, p_send, p_recv, q_send, q_recv,
    y_send, y_recv, z_send, z_recv, sw_send, sw_recv, sh_send, sh_recv,
    wo_send, wo_recv, ho_send, ho_recv, ow_sem, oh_sem,
):
    docs, words = c_v.shape
    topics = w_bf.shape[1]
    dt, vt, kh = docs // ND, words // NV, topics // 2
    half, quarter = dt // 2, dt // 4
    n_dev = rows * cols
    y, i = lax.axis_index("row"), lax.axis_index("col")
    x, core = i // 2, i % 2
    me = y * cols + i
    partner = {"col": x * 2 + (1 - core)}
    across = {"col": (1 - x) * 2 + core}
    above = {"row": 1 - y}

    def peer(step):
        other = (me + step) % n_dev
        return {"row": other // cols, "col": other % cols}

    def rows_at(start, size):
        return pl.ds(pl.multiple_of(start, size), size)

    def remote(src, dst, send, recv, device):
        return pltpu.make_async_remote_copy(
            src_ref=src, dst_ref=dst, send_sem=send, recv_sem=recv, device_id=device, device_id_type=MESH)

    def mine(d):
        return rows_at(d * dt + core * half + x * quarter, quarter)

    def theirs(d):
        return rows_at(d * dt + core * half + (1 - x) * quarter, quarter)

    def copy_a(d):
        return remote(a_w.at[rows_at(d * dt + (1 - core) * half, half)], r_a.at[rows_at(d * half, half)],
                      a_send.at[d], a_recv.at[d], partner)

    def copy_x(d):
        return remote(a_w.at[theirs(d)], r_x.at[rows_at(d * quarter, quarter)], x_send.at[d], x_recv.at[d], across)

    def copy_g(d):
        return remote(w_bf.at[mine(d)], w_bf.at[mine(d)], g_send.at[d], g_recv.at[d], across)

    def copy_p(d):
        return remote(w_bf.at[mine(d)], w_bf.at[mine(d)], p_send.at[d], p_recv.at[d], partner)

    def copy_q(d):
        return remote(w_bf.at[theirs(d)], w_bf.at[theirs(d)], q_send.at[d], q_recv.at[d], partner)

    own_k, other_k = rows_at(y * kh, kh), rows_at((1 - y) * kh, kh)

    def words_at(v):
        return rows_at(v * vt, vt)

    def copy_y(v):
        return remote(a_h.at[v, other_k], r_y.at[v], y_send.at[v], y_recv.at[v], above)

    def copy_z(v):
        return remote(h_bf.at[v, own_k], h_bf.at[v, own_k], z_send.at[v], z_recv.at[v], above)

    def copy_sw(step):
        return remote(sw_acc, sw_slots.at[me], sw_send.at[step - 1], sw_recv.at[step - 1], peer(step))

    def copy_sh(step):
        return remote(sh_part, sh_slots.at[me], sh_send.at[step - 1], sh_recv.at[step - 1], peer(step))

    def copy_wo(d, step):
        k = d * (cols - 1) + step - 1
        return remote(w_f.at[rows_at(d * quarter, quarter)], w_out.at[mine(d)], wo_send.at[k], wo_recv.at[k],
                      {"col": (i + step) % cols})

    def copy_ho(v):
        return remote(h_f.at[v], h_out.at[own_k, words_at(v)], ho_send.at[v], ho_recv.at[v], above)

    def out_w(d):
        return pltpu.make_async_copy(w_f.at[rows_at(d * quarter, quarter)], w_out.at[mine(d)], ow_sem.at[d])

    def out_h(v):
        return pltpu.make_async_copy(h_f.at[v], h_out.at[own_k, words_at(v)], oh_sem.at[v])

    def load_c(d):
        return pltpu.make_async_copy(c_hbm.at[rows_at(d * dt, dt)], c_v.at[rows_at(d * dt, dt)], c_sem.at[d])

    def each(count, body):
        def step(n, carry):
            body(n)
            return carry
        lax.fori_loop(0, count, step, 0)

    def ratio(d, v):
        z = jnp.dot(w_bf[rows_at(d * dt, dt), :], h_bf[v], preferred_element_type=F32)
        return (c_v[rows_at(d * dt, dt), words_at(v)].astype(F32) / (z + EPS)).astype(BF16)

    def select(first, held):
        if isinstance(first, bool):
            return jnp.zeros_like(held) if first else held
        return jnp.where(first, 0.0, held)

    def w_tile(d, v):
        part = jnp.dot(ratio(d, v), h_t[words_at(v), :], preferred_element_type=F32)
        held = a_w[rows_at(d * dt, dt), :]
        a_w[rows_at(d * dt, dt), :] = select(v == 0, held) + part

    def h_tile(d, v):
        part = jnp.dot(w_t[...], ratio(d, v), preferred_element_type=F32)
        held = a_h[v]
        a_h[v] = select(d == 0, held) + part

    def fold_lanes(block):
        total = block[:, :LANES]
        for g in range(1, block.shape[1] // LANES):
            total = total + block[:, g * LANES:(g + 1) * LANES]
        return total

    def send_sh():
        sh_part[...] = jnp.sum(sh_acc[...].T.reshape(LANES // 8, 8, kh), axis=0)
        sh_slots[me] = sh_part[...]
        for step in range(1, n_dev):
            copy_sh(step).start()

    def take_sh():
        for step in range(1, n_dev):
            copy_sh(step).wait()
        for r in range(rows):
            total = sh_slots[r * cols]
            for n in range(1, cols):
                total = total + sh_slots[r * cols + n]
            sh_row[:, r * kh:(r + 1) * kh] = jnp.broadcast_to(jnp.sum(total, axis=0, keepdims=True), (8, kh))

    def send_sw():
        sw_slots[me] = sw_acc[...]
        for step in range(1, n_dev):
            copy_sw(step).start()

    def take_sw():
        for step in range(1, n_dev):
            copy_sw(step).wait()
        total = sw_slots[0]
        for n in range(1, n_dev):
            total = total + sw_slots[n]
        total = jnp.sum(total, axis=0, keepdims=True)
        own = jnp.where(y == 0, total[:, :kh], total[:, kh:])
        sw_col[...] = jnp.broadcast_to(own, (LANES, kh)).T

    def load_h(v):
        return pltpu.make_async_copy(h_hbm.at[:, words_at(v)], a_h.at[v], h_sem.at[v])

    def load_w(d):
        return pltpu.make_async_copy(w_hbm.at[rows_at(d * dt, dt)], a_w.at[rows_at(d * dt, dt)], w_sem.at[d])

    barrier = pltpu.get_barrier_semaphore()
    for step in range(1, n_dev):
        pl.semaphore_signal(barrier, inc=1, device_id=peer(step), device_id_type=MESH)
    each(NV, lambda v: load_h(v).start())
    load_w(0).start()
    load_c(0).start()
    sh_acc[...] = jnp.zeros_like(sh_acc)

    def start_h(v):
        load_h(v).wait()
        h_bf[v] = a_h[v].astype(BF16)
        own = a_h[v, own_k]
        h_f[v] = own
        sh_acc[...] += fold_lanes(own)
        h_t[words_at(v), :] = h_bf[v].T

        @pl.when(v + 1 < ND)
        def _():
            load_w(v + 1).start()
            load_c(v + 1).start()

    each(NV, start_h)
    pl.semaphore_wait(barrier, n_dev - 1)
    send_sh()

    def start_w(d):
        load_w(d).wait()
        w_bf[rows_at(d * dt, dt), :] = a_w[rows_at(d * dt, dt), :].astype(BF16)
        w_f[rows_at(d * quarter, quarter), :] = a_w[mine(d), :]
        load_c(d).wait()

    def sweep_body(sweep, carry):
        last = sweep == SWEEPS - 1

        def s0(d):
            @pl.when(sweep == 0)
            def _():
                start_w(d)
                for v in range(NV):
                    w_tile(d, v)

            @pl.when(sweep > 0)
            def _():
                w_tile(d, NV - 1)
            copy_a(d).start()

        def s1(d):
            copy_a(d).wait_recv()
            own = rows_at(d * dt + core * half, half)
            a_w[own, :] += r_a[rows_at(d * half, half), :]
            copy_x(d).start()

        def s2(d):
            @pl.when(d == 0)
            def _():
                take_sh()
                sw_acc[...] = jnp.zeros_like(sw_acc)
            copy_x(d).wait_recv()
            own = rows_at(d * quarter, quarter)
            fresh = w_f[own, :] * (a_w[mine(d), :] + r_x[own, :]) / sh_row[0:1, :]
            w_f[own, :] = fresh
            w_bf[mine(d), :] = fresh.astype(BF16)
            copy_g(d).start()
            copy_p(d).start()
            sw_acc[...] += jnp.sum(fresh.reshape(quarter // 8, 8, topics), axis=0)

            @pl.when(d == ND - 1)
            def _():
                send_sw()

        def s3(d):
            copy_g(d).wait_recv()
            copy_q(d).start()

        def s5(d):
            copy_p(d).wait_recv()
            copy_q(d).wait_recv()
            w_t[...] = w_bf[rows_at(d * dt, dt), :].T

            @pl.when(d < ND - 1)
            def _():
                for v in range(NV):
                    h_tile(d, v)

            @pl.when(d == ND - 1)
            def _():
                def group(n):
                    h_tile(d, 2 * n)
                    h_tile(d, 2 * n + 1)

                    @pl.when(n == 0)
                    def _():
                        copy_y(0).start()
                        copy_y(1).start()
                each(NV // 2, group)

        def stage(it, lag, body):
            @pl.when(jnp.logical_and(it >= lag, it < lag + ND))
            def _():
                body(it - lag)

        def w_step(it):
            for lag, body in ((LAG2, s2), (LAG1, s1), (0, s0), (LAG3, s3), (LAG5, s5)):
                stage(it, lag, body)

        each(ND + LAG5, w_step)

        def w_sent(d):
            copy_a(d).wait_send()
            copy_x(d).wait_send()
            copy_g(d).wait_send()
            copy_p(d).wait_send()
            copy_q(d).wait_send()

        each(ND, w_sent)

        @pl.when(last)
        def _():
            def give(d):
                out_w(d).start()
                for step in range(1, cols):
                    copy_wo(d, step).start()
            each(ND, give)

        def t1(v):
            @pl.when(v == 0)
            def _():
                take_sw()
                sh_acc[...] = jnp.zeros_like(sh_acc)
            copy_y(v).wait_recv()
            for g in range(vt // LANES):
                at = slice(g * LANES, (g + 1) * LANES)
                fresh = h_f[v, :, at] * (a_h[v, own_k, at] + r_y[v, :, at]) / sw_col[...]
                h_f[v, :, at] = fresh
                h_bf[v, own_k, at] = fresh.astype(BF16)
                sh_acc[...] += fresh

            @pl.when(jnp.logical_not(last))
            def _():
                copy_z(v).start()

                @pl.when(v == NV - 1)
                def _():
                    send_sh()

            @pl.when(last)
            def _():
                out_h(v).start()
                copy_ho(v).start()

            @pl.when(v + 2 < NV)
            def _():
                copy_y(v + 2).start()

        def t3(v):
            copy_z(v).wait_recv()
            h_t[words_at(v), :] = h_bf[v].T

            @pl.when(v < NV - 1)
            def _():
                def group(n):
                    for k in range(GROUP):
                        w_tile(n * GROUP + k, v)
                each(ND // GROUP, group)

        def h_step(it):
            @pl.when(it < NV)
            def _():
                t1(it)

            @pl.when(jnp.logical_and(it >= 1, jnp.logical_not(last)))
            def _():
                t3(it - 1)

        each(NV + 1, h_step)

        def h_sent(v):
            copy_y(v).wait_send()

            @pl.when(jnp.logical_not(last))
            def _():
                copy_z(v).wait_send()

        each(NV, h_sent)
        return carry

    lax.fori_loop(0, SWEEPS, sweep_body, 0)

    def finish_w(d):
        out_w(d).wait()
        for step in range(1, cols):
            copy_wo(d, step).wait()

    def finish_h(v):
        out_h(v).wait()
        copy_ho(v).wait()

    each(ND, finish_w)
    each(NV, finish_h)


def solution(mesh):
    rows, cols = mesh.shape["row"], mesh.shape["col"]
    n_dev = rows * cols

    def local(c_blk, w_loc, h_loc):
        docs, words = c_blk.shape
        topics = w_loc.shape[1]
        vmem = pltpu.VMEM
        dma = pltpu.SemaphoreType.DMA
        scratch = [
            vmem((docs, words), BF16),
            vmem((docs, topics), BF16),
            vmem((topics, docs // ND), BF16),
            vmem((NV, topics, words // NV), BF16),
            vmem((words, topics), BF16),
            vmem((docs // 4, topics), F32),
            vmem((NV, topics // 2, words // NV), F32),
            vmem((docs, topics), F32),
            vmem((NV, topics, words // NV), F32),
            vmem((docs // 2, topics), F32),
            vmem((docs // 4, topics), F32),
            vmem((NV, topics // 2, words // NV), F32),
            vmem((8, topics), F32),
            vmem((n_dev, 8, topics), F32),
            vmem((topics // 2, LANES), F32),
            vmem((topics // 2, LANES), F32),
            vmem((8, topics // 2), F32),
            vmem((n_dev, 8, topics // 2), F32),
            vmem((8, topics), F32),
            dma((ND,)),
            dma((NV,)),
            dma((ND,)),
        ]
        scratch += [dma((ND,))] * 10
        scratch += [dma((NV,))] * 4
        scratch += [dma((n_dev - 1,))] * 4
        scratch += [dma((ND * (cols - 1),))] * 2
        scratch += [dma((NV,))] * 2
        scratch += [dma((ND,)), dma((NV,))]
        any_space = pl.BlockSpec(memory_space=pl.ANY)
        return pl.pallas_call(
            functools.partial(kernel, rows, cols),
            out_shape=(jax.ShapeDtypeStruct(w_loc.shape, F32), jax.ShapeDtypeStruct(h_loc.shape, F32)),
            in_specs=[any_space] * 3,
            out_specs=(any_space, any_space),
            scratch_shapes=scratch,
            compiler_params=pltpu.CompilerParams(
                collective_id=0, has_side_effects=True, vmem_limit_bytes=67_043_328),
            name="nmf",
        )(c_blk, w_loc, h_loc)

    spec_c = P(("part", "row"), "col")
    spec_w = P(("part", "row"), None)
    spec_h = P(None, ("part", "col"))
    return jax.shard_map(local, mesh=mesh, in_specs=(spec_c, spec_w, spec_h), out_specs=(spec_w, spec_h), check_vma=False)
```

```python
import functools

import jax
import jax.numpy as jnp
from jax import lax
from jax.experimental import pallas as pl
from jax.experimental.pallas import tpu as pltpu
from jax.sharding import PartitionSpec as P

SWEEPS = 4
EPS = 1e-6
ND = 8
NV = 8
GROUP = 4
S_OTHER = 4
LAG1, LAG2, LAG3, LAG5 = 2, 4, 5, 6
LANES = 128
MESH = pl.DeviceIdType.MESH
F32 = jnp.float32
BF16 = jnp.bfloat16


def kernel(
    rows, cols, c_hbm, w_hbm, h_hbm, w_out, h_out,
    c_v, w_bf, w_t, h_bf, h_t, w_f, h_f, a_w, a_h, r_a, r_x, r_y,
    sw_acc, sw_slots, sw_col, sh_acc, sh_part, sh_slots, sh_row,
    c_two, w_two, a_s, h_s, c_send, c_recv, u_send, u_recv, b_send, b_recv, s_sems, os_sem,
    w_sem, h_sem, c_sem,
    a_send, a_recv, x_send, x_recv, g_send, g_recv, p_send, p_recv, q_send, q_recv,
    y_send, y_recv, z_send, z_recv, sw_send, sw_recv, sh_send, sh_recv,
    wo_send, wo_recv, ho_send, ho_recv, ow_sem, oh_sem,
):
    docs, words = c_v.shape
    topics = w_bf.shape[1]
    dt, vt, kh = docs // ND, words // NV, topics // 2
    half, quarter = dt // 2, dt // 4
    nr, vh = NV - 1, vt // 2
    n_dev = rows * cols
    y, i = lax.axis_index("row"), lax.axis_index("col")
    x, core = i // 2, i % 2
    me = y * cols + i
    partner = {"col": x * 2 + (1 - core)}
    across = {"col": (1 - x) * 2 + core}
    above = {"row": 1 - y}

    def peer(step):
        other = (me + step) % n_dev
        return {"row": other // cols, "col": other % cols}

    def rows_at(start, size):
        return pl.ds(pl.multiple_of(start, size), size)

    def remote(src, dst, send, recv, device):
        return pltpu.make_async_remote_copy(
            src_ref=src, dst_ref=dst, send_sem=send, recv_sem=recv, device_id=device, device_id_type=MESH)

    def mine(d):
        return rows_at(d * dt + core * half + x * quarter, quarter)

    def theirs(d):
        return rows_at(d * dt + core * half + (1 - x) * quarter, quarter)

    def copy_a(d):
        return remote(a_w.at[rows_at(d * dt + (1 - core) * half, half)], r_a.at[rows_at(d * half, half)],
                      a_send.at[d], a_recv.at[d], partner)

    def copy_x(d):
        return remote(a_w.at[theirs(d)], r_x.at[rows_at(d * quarter, quarter)], x_send.at[d], x_recv.at[d], across)

    def copy_g(d):
        return remote(w_bf.at[mine(d)], w_bf.at[mine(d)], g_send.at[d], g_recv.at[d], across)

    def copy_p(d):
        return remote(w_bf.at[mine(d)], w_bf.at[mine(d)], p_send.at[d], p_recv.at[d], partner)

    def copy_q(d):
        return remote(w_bf.at[theirs(d)], w_bf.at[theirs(d)], q_send.at[d], q_recv.at[d], partner)

    own_k, other_k = rows_at(y * kh, kh), rows_at((1 - y) * kh, kh)

    def words_at(v):
        return rows_at(v * vt, vt)

    def copy_y(v):
        return remote(a_h.at[v, other_k], r_y.at[v], y_send.at[v], y_recv.at[v], above)

    def copy_z(v):
        return remote(h_bf.at[v, own_k], h_bf.at[v, own_k], z_send.at[v], z_recv.at[v], above)

    def shared(side):
        return rows_at(side * vh, vh)

    def whole(side):
        return rows_at(nr * vt + side * vh, vh)

    def copy_c():
        return remote(c_hbm.at[:, whole(1 - y)], c_two, c_send.at[0], c_recv.at[0], above)

    def copy_u(d):
        return remote(w_bf.at[mine(d)], w_two.at[d, core * 2 + x], u_send.at[d], u_recv.at[d], above)

    def copy_b(step):
        strip = w_two.at[:, core * 2 + x]
        return remote(strip, strip, b_send.at[step - 1], b_recv.at[step - 1], {"col": (i + step) % cols})

    def copy_zs():
        return remote(h_bf.at[nr, :, shared(y)], h_bf.at[nr, :, shared(y)], s_sems.at[0], s_sems.at[1], above)

    def copy_hs():
        return remote(h_s, h_out.at[:, whole(y)], s_sems.at[2], s_sems.at[3], above)

    def out_s():
        return pltpu.make_async_copy(h_s, h_out.at[:, whole(y)], os_sem.at[0])

    def copy_sw(step):
        return remote(sw_acc, sw_slots.at[me], sw_send.at[step - 1], sw_recv.at[step - 1], peer(step))

    def copy_sh(step):
        return remote(sh_part, sh_slots.at[me], sh_send.at[step - 1], sh_recv.at[step - 1], peer(step))

    def copy_wo(d, step):
        k = d * (cols - 1) + step - 1
        return remote(w_f.at[rows_at(d * quarter, quarter)], w_out.at[mine(d)], wo_send.at[k], wo_recv.at[k],
                      {"col": (i + step) % cols})

    def copy_ho(v):
        return remote(h_f.at[v], h_out.at[own_k, words_at(v)], ho_send.at[v], ho_recv.at[v], above)

    def out_w(d):
        return pltpu.make_async_copy(w_f.at[rows_at(d * quarter, quarter)], w_out.at[mine(d)], ow_sem.at[d])

    def out_h(v):
        return pltpu.make_async_copy(h_f.at[v], h_out.at[own_k, words_at(v)], oh_sem.at[v])

    def load_c(d):
        return pltpu.make_async_copy(c_hbm.at[rows_at(d * dt, dt)], c_v.at[rows_at(d * dt, dt)], c_sem.at[d])

    def each(count, body):
        def step(n, carry):
            body(n)
            return carry
        lax.fori_loop(0, count, step, 0)

    def ratio(d, v):
        z = jnp.dot(w_bf[rows_at(d * dt, dt), :], h_bf[v], preferred_element_type=F32)
        return (c_v[rows_at(d * dt, dt), words_at(v)].astype(F32) / (z + EPS)).astype(BF16)

    def select(first, held):
        if isinstance(first, bool):
            return jnp.zeros_like(held) if first else held
        return jnp.where(first, 0.0, held)

    def w_tile(d, v):
        part = jnp.dot(ratio(d, v), h_t[words_at(v), :], preferred_element_type=F32)
        held = a_w[rows_at(d * dt, dt), :]
        a_w[rows_at(d * dt, dt), :] = select(v == 0, held) + part

    def h_tile(d, v):
        part = jnp.dot(w_t[...], ratio(d, v), preferred_element_type=F32)
        held = a_h[v]
        a_h[v] = select(d == 0, held) + part

    def s_tile(d, rows_bf, counts, first):
        z = jnp.dot(rows_bf, h_bf[nr, :, shared(y)], preferred_element_type=F32)
        q = (counts.astype(F32) / (z + EPS)).astype(BF16)
        part = jnp.dot(rows_bf.T, q, preferred_element_type=F32)
        a_s[...] = (jnp.where(d == 0, 0.0, a_s[...]) if first else a_s[...]) + part

    def s_own(d):
        at = rows_at(d * dt, dt)
        s_tile(d, w_bf[at, :], c_v[at, whole(y)], True)

    def s_other(d):
        s_tile(d, w_two[d].reshape(dt, topics), c_two[rows_at(d * dt, dt), :], False)

    def fold_lanes(block):
        total = block[:, :LANES]
        for g in range(1, block.shape[1] // LANES):
            total = total + block[:, g * LANES:(g + 1) * LANES]
        return total

    def send_sh():
        for r in range(rows):
            at = slice(r * kh, (r + 1) * kh)
            sh_part[:, at] = jnp.sum(sh_acc[at, :].T.reshape(LANES // 8, 8, kh), axis=0)
        sh_slots[me] = sh_part[...]
        for step in range(1, n_dev):
            copy_sh(step).start()

    def take_sh():
        for step in range(1, n_dev):
            copy_sh(step).wait()
        total = sh_slots[0]
        for n in range(1, n_dev):
            total = total + sh_slots[n]
        sh_row[...] = jnp.broadcast_to(jnp.sum(total, axis=0, keepdims=True), (8, topics))

    def send_sw():
        sw_slots[me] = sw_acc[...]
        for step in range(1, n_dev):
            copy_sw(step).start()

    def take_sw():
        for step in range(1, n_dev):
            copy_sw(step).wait()
        total = sw_slots[0]
        for n in range(1, n_dev):
            total = total + sw_slots[n]
        total = jnp.sum(total, axis=0, keepdims=True)
        for r in range(rows):
            at = slice(r * kh, (r + 1) * kh)
            sw_col[at, :] = jnp.broadcast_to(total[:, at], (LANES, kh)).T

    def load_h(v):
        return pltpu.make_async_copy(h_hbm.at[:, words_at(v)], a_h.at[v], h_sem.at[v])

    def load_w(d):
        return pltpu.make_async_copy(w_hbm.at[rows_at(d * dt, dt)], a_w.at[rows_at(d * dt, dt)], w_sem.at[d])

    barrier = pltpu.get_barrier_semaphore()
    for step in range(1, n_dev):
        pl.semaphore_signal(barrier, inc=1, device_id=peer(step), device_id_type=MESH)
    each(NV, lambda v: load_h(v).start())
    load_w(0).start()
    load_c(0).start()
    sh_acc[...] = jnp.zeros_like(sh_acc)

    def start_h(v):
        load_h(v).wait()
        h_bf[v] = a_h[v].astype(BF16)
        h_t[words_at(v), :] = h_bf[v].T

        @pl.when(v < nr)
        def _():
            own = a_h[v, own_k]
            h_f[v] = own
            sh_acc[own_k, :] += fold_lanes(own)

        @pl.when(v == nr)
        def _():
            own = a_h[nr, :, shared(y)]
            h_s[...] = own
            sh_acc[...] += fold_lanes(own)

        @pl.when(v + 1 < ND)
        def _():
            load_w(v + 1).start()
            load_c(v + 1).start()

    each(NV, start_h)
    pl.semaphore_wait(barrier, n_dev - 1)
    send_sh()
    copy_c().start()

    def start_w(d):
        load_w(d).wait()
        w_bf[rows_at(d * dt, dt), :] = a_w[rows_at(d * dt, dt), :].astype(BF16)
        w_f[rows_at(d * quarter, quarter), :] = a_w[mine(d), :]
        load_c(d).wait()

    def sweep_body(sweep, carry):
        last = sweep == SWEEPS - 1

        def s0(d):
            @pl.when(sweep == 0)
            def _():
                start_w(d)
                for v in range(NV):
                    w_tile(d, v)

            @pl.when(sweep > 0)
            def _():
                w_tile(d, nr - 1)
            copy_a(d).start()

        def s1(d):
            copy_a(d).wait_recv()
            own = rows_at(d * dt + core * half, half)
            a_w[own, :] += r_a[rows_at(d * half, half), :]
            copy_x(d).start()

        def s2(d):
            @pl.when(d == 0)
            def _():
                take_sh()
                sw_acc[...] = jnp.zeros_like(sw_acc)
            copy_x(d).wait_recv()
            own = rows_at(d * quarter, quarter)
            fresh = w_f[own, :] * (a_w[mine(d), :] + r_x[own, :]) / sh_row[0:1, :]
            w_f[own, :] = fresh
            w_bf[mine(d), :] = fresh.astype(BF16)
            copy_g(d).start()
            copy_p(d).start()

            @pl.when(sweep > 0)
            def _():
                copy_u(d).start()
            sw_acc[...] += jnp.sum(fresh.reshape(quarter // 8, 8, topics), axis=0)

            @pl.when(d == ND - 1)
            def _():
                send_sw()

        def s3(d):
            copy_g(d).wait_recv()
            copy_q(d).start()

        def s5(d):
            copy_p(d).wait_recv()
            copy_q(d).wait_recv()
            w_t[...] = w_bf[rows_at(d * dt, dt), :].T

            @pl.when(d < ND - 1)
            def _():
                for v in range(nr):
                    h_tile(d, v)

            @pl.when(d == ND - 1)
            def _():
                h_tile(d, 0)
                h_tile(d, 1)
                copy_y(0).start()
                copy_y(1).start()
                for v in range(2, nr):
                    h_tile(d, v)

        def stage(it, lag, body):
            @pl.when(jnp.logical_and(it >= lag, it < lag + ND))
            def _():
                body(it - lag)

        def w_step(it):
            for lag, body in ((LAG2, s2), (LAG1, s1), (0, s0), (LAG3, s3), (LAG5, s5)):
                stage(it, lag, body)

        each(ND + LAG5, w_step)

        def w_sent(d):
            copy_a(d).wait_send()
            copy_x(d).wait_send()
            copy_g(d).wait_send()
            copy_p(d).wait_send()
            copy_q(d).wait_send()

        each(ND, w_sent)

        @pl.when(last)
        def _():
            def give(d):
                out_w(d).start()
                for step in range(1, cols):
                    copy_wo(d, step).start()
            each(ND, give)

        def t1(v):
            @pl.when(v == 0)
            def _():
                take_sw()
                sh_acc[...] = jnp.zeros_like(sh_acc)
            copy_y(v).wait_recv()
            for g in range(vt // LANES):
                at = slice(g * LANES, (g + 1) * LANES)
                fresh = h_f[v, :, at] * (a_h[v, own_k, at] + r_y[v, :, at]) / sw_col[own_k, :]
                h_f[v, :, at] = fresh
                h_bf[v, own_k, at] = fresh.astype(BF16)
                sh_acc[own_k, :] += fresh

            @pl.when(jnp.logical_not(last))
            def _():
                copy_z(v).start()

                @pl.when(v == nr - 1)
                def _():
                    send_sh()

            @pl.when(last)
            def _():
                out_h(v).start()
                copy_ho(v).start()

            @pl.when(v + 2 < nr)
            def _():
                copy_y(v + 2).start()

        def w_words(v):
            def group(n):
                for k in range(GROUP):
                    w_tile(n * GROUP + k, v)
            each(ND // GROUP, group)

        def t3(v):
            copy_z(v).wait_recv()
            h_t[words_at(v), :] = h_bf[v].T

            @pl.when(v < nr - 1)
            def _():
                w_words(v)

        def update_s():
            for g in range(vh // LANES):
                at = slice(g * LANES, (g + 1) * LANES)
                fresh = h_s[:, at] * a_s[:, at] / sw_col[...]
                h_s[:, at] = fresh
                sh_acc[...] += fresh
            h_bf[nr, :, shared(y)] = h_s[...].astype(BF16)

            @pl.when(jnp.logical_not(last))
            def _():
                copy_zs().start()

            @pl.when(last)
            def _():
                out_s().start()
                copy_hs().start()

        def h_step(it):
            @pl.when(it < nr)
            def _():
                t1(it)

            @pl.when(jnp.logical_and(it >= 1, jnp.logical_not(last)))
            def _():
                t3(it - 1)

            @pl.when(it == 1)
            def _():
                each(ND, lambda d: copy_u(d).wait_recv())
                for step in range(1, cols):
                    copy_b(step).start()
                each(ND, s_own)

            @pl.when(it == S_OTHER)
            def _():
                @pl.when(sweep == 0)
                def _():
                    copy_c().wait()
                for step in range(1, cols):
                    copy_b(step).wait()
                each(ND, s_other)

            @pl.when(it == S_OTHER + 1)
            def _():
                update_s()

            @pl.when(jnp.logical_and(it == nr - 1, jnp.logical_not(last)))
            def _():
                copy_zs().wait_recv()
                h_t[words_at(nr), :] = h_bf[nr].T
                w_words(nr)

        @pl.when(sweep == 0)
        def _():
            each(ND, lambda d: copy_u(d).start())

        each(nr + 1, h_step)

        def h_sent(v):
            copy_y(v).wait_send()

            @pl.when(jnp.logical_not(last))
            def _():
                copy_z(v).wait_send()

        each(nr, h_sent)
        each(ND, lambda d: copy_u(d).wait_send())

        @pl.when(jnp.logical_not(last))
        def _():
            copy_zs().wait_send()
        return carry

    lax.fori_loop(0, SWEEPS, sweep_body, 0)

    def finish_w(d):
        out_w(d).wait()
        for step in range(1, cols):
            copy_wo(d, step).wait()

    def finish_h(v):
        out_h(v).wait()
        copy_ho(v).wait()

    each(ND, finish_w)
    each(nr, finish_h)
    out_s().wait()
    copy_hs().wait()


def solution(mesh):
    rows, cols = mesh.shape["row"], mesh.shape["col"]
    n_dev = rows * cols

    def local(c_blk, w_loc, h_loc):
        docs, words = c_blk.shape
        topics = w_loc.shape[1]
        vmem = pltpu.VMEM
        dma = pltpu.SemaphoreType.DMA
        chunk = words // NV
        scratch = [
            vmem((docs, words), BF16),
            vmem((docs, topics), BF16),
            vmem((topics, docs // ND), BF16),
            vmem((NV, topics, chunk), BF16),
            vmem((words, topics), BF16),
            vmem((docs // 4, topics), F32),
            vmem((NV - 1, topics // 2, chunk), F32),
            vmem((docs, topics), F32),
            vmem((NV, topics, chunk), F32),
            vmem((docs // 2, topics), F32),
            vmem((docs // 4, topics), F32),
            vmem((NV - 1, topics // 2, chunk), F32),
            vmem((8, topics), F32),
            vmem((n_dev, 8, topics), F32),
            vmem((topics, LANES), F32),
            vmem((topics, LANES), F32),
            vmem((8, topics), F32),
            vmem((n_dev, 8, topics), F32),
            vmem((8, topics), F32),
            vmem((docs, chunk // 2), BF16),
            vmem((ND, 4, docs // ND // 4, topics), BF16),
            vmem((topics, chunk // 2), F32),
            vmem((topics, chunk // 2), F32),
        ]
        sizes = [1, 1, ND, ND, cols - 1, cols - 1, 4, 1, ND, NV, ND]
        sizes += [ND] * 10 + [NV] * 4 + [n_dev - 1] * 4 + [ND * (cols - 1)] * 2 + [NV] * 2 + [ND, NV]
        scratch += [dma((size,)) for size in sizes]
        any_space = pl.BlockSpec(memory_space=pl.ANY)
        return pl.pallas_call(
            functools.partial(kernel, rows, cols),
            out_shape=(jax.ShapeDtypeStruct(w_loc.shape, F32), jax.ShapeDtypeStruct(h_loc.shape, F32)),
            in_specs=[any_space] * 3,
            out_specs=(any_space, any_space),
            scratch_shapes=scratch,
            compiler_params=pltpu.CompilerParams(
                collective_id=0, has_side_effects=True, vmem_limit_bytes=67_043_328),
            name="nmf",
        )(c_blk, w_loc, h_loc)

    spec_c = P(("part", "row"), "col")
    spec_w = P(("part", "row"), None)
    spec_h = P(None, ("part", "col"))
    return jax.shard_map(local, mesh=mesh, in_specs=(spec_c, spec_w, spec_h), out_specs=(spec_w, spec_h), check_vma=False)
```

```python
import functools

import jax
import jax.numpy as jnp
from jax import lax
from jax.experimental import pallas as pl
from jax.experimental.pallas import tpu as pltpu
from jax.sharding import PartitionSpec as P

SWEEPS = 4
EPS = 1e-6
ND = 8
NV = 8
GROUP = 4
S_OTHER = 3
LAG1, LAG2, LAG3, LAG5 = 2, 4, 5, 6
LANES = 128
MESH = pl.DeviceIdType.MESH
F32 = jnp.float32
BF16 = jnp.bfloat16


def kernel(
    rows, cols, c_hbm, w_hbm, h_hbm, w_out, h_out,
    c_v, w_bf, w_t, h_bf, h_t, w_f, h_f, a_w, a_h, r_a, r_x, r_y,
    sw_acc, sw_slots, sw_col, sh_acc, sh_part, sh_slots, sh_row,
    c_two, w_two, a_s, h_s, c_send, c_recv, u_send, u_recv, b_send, b_recv, s_sems, os_sem,
    w_sem, h_sem, c_sem,
    a_send, a_recv, x_send, x_recv, g_send, g_recv, p_send, p_recv, q_send, q_recv,
    y_send, y_recv, z_send, z_recv, sw_send, sw_recv, sh_send, sh_recv,
    wo_send, wo_recv, ho_send, ho_recv, ow_sem, oh_sem,
):
    docs, words = c_v.shape
    topics = w_bf.shape[1]
    dt, vt, kh = docs // ND, words // NV, topics // 2
    half, quarter = dt // 2, dt // 4
    nr, vh = NV - 1, vt // 2
    n_dev = rows * cols
    y, i = lax.axis_index("row"), lax.axis_index("col")
    x, core = i // 2, i % 2
    me = y * cols + i
    partner = {"col": x * 2 + (1 - core)}
    across = {"col": (1 - x) * 2 + core}
    above = {"row": 1 - y}

    def peer(step):
        other = (me + step) % n_dev
        return {"row": other // cols, "col": other % cols}

    def rows_at(start, size):
        return pl.ds(pl.multiple_of(start, size), size)

    def remote(src, dst, send, recv, device):
        return pltpu.make_async_remote_copy(
            src_ref=src, dst_ref=dst, send_sem=send, recv_sem=recv, device_id=device, device_id_type=MESH)

    def mine(d):
        return rows_at(d * dt + core * half + x * quarter, quarter)

    def theirs(d):
        return rows_at(d * dt + core * half + (1 - x) * quarter, quarter)

    def copy_a(d):
        return remote(a_w.at[rows_at(d * dt + (1 - core) * half, half)], r_a.at[rows_at(d * half, half)],
                      a_send.at[d], a_recv.at[d], partner)

    def copy_x(d):
        return remote(a_w.at[theirs(d)], r_x.at[rows_at(d * quarter, quarter)], x_send.at[d], x_recv.at[d], across)

    def copy_g(d):
        return remote(w_bf.at[mine(d)], w_bf.at[mine(d)], g_send.at[d], g_recv.at[d], across)

    def copy_p(d):
        return remote(w_bf.at[mine(d)], w_bf.at[mine(d)], p_send.at[d], p_recv.at[d], partner)

    def copy_q(d):
        return remote(w_bf.at[theirs(d)], w_bf.at[theirs(d)], q_send.at[d], q_recv.at[d], partner)

    own_k, other_k = rows_at(y * kh, kh), rows_at((1 - y) * kh, kh)

    def words_at(v):
        return rows_at(v * vt, vt)

    def copy_y(v):
        return remote(a_h.at[v, other_k], r_y.at[v], y_send.at[v], y_recv.at[v], above)

    def copy_z(v):
        return remote(h_bf.at[v, own_k], h_bf.at[v, own_k], z_send.at[v], z_recv.at[v], above)

    def shared(side):
        return rows_at(side * vh, vh)

    def whole(side):
        return rows_at(nr * vt + side * vh, vh)

    def copy_c():
        return remote(c_hbm.at[:, whole(1 - y)], c_two, c_send.at[0], c_recv.at[0], above)

    def copy_u(d):
        return remote(w_bf.at[mine(d)], w_two.at[d, core * 2 + x], u_send.at[d], u_recv.at[d], above)

    def copy_b(step):
        strip = w_two.at[:, core * 2 + x]
        return remote(strip, strip, b_send.at[step - 1], b_recv.at[step - 1], {"col": (i + step) % cols})

    def copy_zs():
        return remote(h_bf.at[nr, :, shared(y)], h_bf.at[nr, :, shared(y)], s_sems.at[0], s_sems.at[1], above)

    def copy_hs():
        return remote(h_s, h_out.at[:, whole(y)], s_sems.at[2], s_sems.at[3], above)

    def out_s():
        return pltpu.make_async_copy(h_s, h_out.at[:, whole(y)], os_sem.at[0])

    def copy_sw(step):
        return remote(sw_acc, sw_slots.at[me], sw_send.at[step - 1], sw_recv.at[step - 1], peer(step))

    def copy_sh(step):
        return remote(sh_part, sh_slots.at[me], sh_send.at[step - 1], sh_recv.at[step - 1], peer(step))

    def copy_wo(d, step):
        k = d * (cols - 1) + step - 1
        return remote(w_f.at[rows_at(d * quarter, quarter)], w_out.at[mine(d)], wo_send.at[k], wo_recv.at[k],
                      {"col": (i + step) % cols})

    def copy_ho(v):
        return remote(h_f.at[v], h_out.at[own_k, words_at(v)], ho_send.at[v], ho_recv.at[v], above)

    def out_w(d):
        return pltpu.make_async_copy(w_f.at[rows_at(d * quarter, quarter)], w_out.at[mine(d)], ow_sem.at[d])

    def out_h(v):
        return pltpu.make_async_copy(h_f.at[v], h_out.at[own_k, words_at(v)], oh_sem.at[v])

    def load_c(d):
        return pltpu.make_async_copy(c_hbm.at[rows_at(d * dt, dt)], c_v.at[rows_at(d * dt, dt)], c_sem.at[d])

    def each(count, body):
        def step(n, carry):
            body(n)
            return carry
        lax.fori_loop(0, count, step, 0)

    def ratio(d, v):
        z = jnp.dot(w_bf[rows_at(d * dt, dt), :], h_bf[v], preferred_element_type=F32)
        return (c_v[rows_at(d * dt, dt), words_at(v)].astype(F32) / (z + EPS)).astype(BF16)

    def select(first, held):
        if isinstance(first, bool):
            return jnp.zeros_like(held) if first else held
        return jnp.where(first, 0.0, held)

    def w_tile(d, v):
        part = jnp.dot(ratio(d, v), h_t[words_at(v), :], preferred_element_type=F32)
        held = a_w[rows_at(d * dt, dt), :]
        a_w[rows_at(d * dt, dt), :] = select(v == 0, held) + part

    def h_tile(d, v):
        part = jnp.dot(w_t[...], ratio(d, v), preferred_element_type=F32)
        held = a_h[v]
        a_h[v] = select(d == 0, held) + part

    def s_tile(d, rows_bf, counts, first):
        z = jnp.dot(rows_bf, h_bf[nr, :, shared(y)], preferred_element_type=F32)
        q = (counts.astype(F32) / (z + EPS)).astype(BF16)
        part = jnp.dot(rows_bf.T, q, preferred_element_type=F32)
        a_s[...] = (jnp.where(d == 0, 0.0, a_s[...]) if first else a_s[...]) + part

    def s_own(d):
        at = rows_at(d * dt, dt)
        s_tile(d, w_bf[at, :], c_v[at, whole(y)], True)

    def s_other(d):
        s_tile(d, w_two[d].reshape(dt, topics), c_two[rows_at(d * dt, dt), :], False)

    def fold_lanes(block):
        total = block[:, :LANES]
        for g in range(1, block.shape[1] // LANES):
            total = total + block[:, g * LANES:(g + 1) * LANES]
        return total

    def send_sh():
        for r in range(rows):
            at = slice(r * kh, (r + 1) * kh)
            sh_part[:, at] = jnp.sum(sh_acc[at, :].T.reshape(LANES // 8, 8, kh), axis=0)
        sh_slots[me] = sh_part[...]
        for step in range(1, n_dev):
            copy_sh(step).start()

    def take_sh():
        for step in range(1, n_dev):
            copy_sh(step).wait()
        total = sh_slots[0]
        for n in range(1, n_dev):
            total = total + sh_slots[n]
        sh_row[...] = jnp.broadcast_to(jnp.sum(total, axis=0, keepdims=True), (8, topics))

    def send_sw():
        sw_slots[me] = sw_acc[...]
        for step in range(1, n_dev):
            copy_sw(step).start()

    def take_sw():
        for step in range(1, n_dev):
            copy_sw(step).wait()
        total = sw_slots[0]
        for n in range(1, n_dev):
            total = total + sw_slots[n]
        total = jnp.sum(total, axis=0, keepdims=True)
        for r in range(rows):
            at = slice(r * kh, (r + 1) * kh)
            sw_col[at, :] = jnp.broadcast_to(total[:, at], (LANES, kh)).T

    def load_h(v):
        return pltpu.make_async_copy(h_hbm.at[:, words_at(v)], a_h.at[v], h_sem.at[v])

    def load_w(d):
        return pltpu.make_async_copy(w_hbm.at[rows_at(d * dt, dt)], a_w.at[rows_at(d * dt, dt)], w_sem.at[d])

    barrier = pltpu.get_barrier_semaphore()
    for step in range(1, n_dev):
        pl.semaphore_signal(barrier, inc=1, device_id=peer(step), device_id_type=MESH)
    each(NV, lambda v: load_h(v).start())
    load_w(0).start()
    load_c(0).start()
    sh_acc[...] = jnp.zeros_like(sh_acc)

    def start_h(v):
        load_h(v).wait()
        h_bf[v] = a_h[v].astype(BF16)
        h_t[words_at(v), :] = h_bf[v].T

        @pl.when(v < nr)
        def _():
            own = a_h[v, own_k]
            h_f[v] = own
            sh_acc[own_k, :] += fold_lanes(own)

        @pl.when(v == nr)
        def _():
            own = a_h[nr, :, shared(y)]
            h_s[...] = own
            sh_acc[...] += fold_lanes(own)

        @pl.when(v + 1 < ND)
        def _():
            load_w(v + 1).start()
            load_c(v + 1).start()

    each(NV, start_h)
    pl.semaphore_wait(barrier, n_dev - 1)
    send_sh()
    copy_c().start()

    def start_w(d):
        load_w(d).wait()
        w_bf[rows_at(d * dt, dt), :] = a_w[rows_at(d * dt, dt), :].astype(BF16)
        w_f[rows_at(d * quarter, quarter), :] = a_w[mine(d), :]
        load_c(d).wait()

    def sweep_body(sweep, carry):
        last = sweep == SWEEPS - 1

        def s0(d):
            @pl.when(sweep == 0)
            def _():
                start_w(d)
                for v in range(NV):
                    w_tile(d, v)

            @pl.when(sweep > 0)
            def _():
                w_tile(d, nr - 1)
            copy_a(d).start()

        def s1(d):
            copy_a(d).wait_recv()
            own = rows_at(d * dt + core * half, half)
            a_w[own, :] += r_a[rows_at(d * half, half), :]
            copy_x(d).start()

        def s2(d):
            @pl.when(d == 0)
            def _():
                take_sh()
                sw_acc[...] = jnp.zeros_like(sw_acc)
            copy_x(d).wait_recv()
            own = rows_at(d * quarter, quarter)
            fresh = w_f[own, :] * (a_w[mine(d), :] + r_x[own, :]) / sh_row[0:1, :]
            w_f[own, :] = fresh
            w_bf[mine(d), :] = fresh.astype(BF16)
            copy_g(d).start()
            copy_p(d).start()

            @pl.when(sweep > 0)
            def _():
                copy_u(d).start()
            sw_acc[...] += jnp.sum(fresh.reshape(quarter // 8, 8, topics), axis=0)

            @pl.when(d == ND - 1)
            def _():
                send_sw()

        def s3(d):
            copy_g(d).wait_recv()
            copy_q(d).start()

        def s5(d):
            copy_p(d).wait_recv()
            copy_q(d).wait_recv()
            w_t[...] = w_bf[rows_at(d * dt, dt), :].T

            @pl.when(d < ND - 1)
            def _():
                for v in range(nr):
                    h_tile(d, v)

            @pl.when(d == ND - 1)
            def _():
                h_tile(d, 0)
                h_tile(d, 1)
                copy_y(0).start()
                copy_y(1).start()
                for v in range(2, nr):
                    h_tile(d, v)

        def stage(it, lag, body):
            @pl.when(jnp.logical_and(it >= lag, it < lag + ND))
            def _():
                body(it - lag)

        def w_step(it):
            for lag, body in ((LAG2, s2), (LAG1, s1), (0, s0), (LAG3, s3), (LAG5, s5)):
                stage(it, lag, body)

        each(ND + LAG5, w_step)

        def w_sent(d):
            copy_a(d).wait_send()
            copy_x(d).wait_send()
            copy_g(d).wait_send()
            copy_p(d).wait_send()
            copy_q(d).wait_send()

        each(ND, w_sent)

        def give(d):
            out_w(d).start()
            for step in range(1, cols):
                copy_wo(d, step).start()

        def t1(v):
            @pl.when(v == 0)
            def _():
                take_sw()
                sh_acc[...] = jnp.zeros_like(sh_acc)
            copy_y(v).wait_recv()
            for g in range(vt // LANES):
                at = slice(g * LANES, (g + 1) * LANES)
                fresh = h_f[v, :, at] * (a_h[v, own_k, at] + r_y[v, :, at]) / sw_col[own_k, :]
                h_f[v, :, at] = fresh
                h_bf[v, own_k, at] = fresh.astype(BF16)
                sh_acc[own_k, :] += fresh

            @pl.when(jnp.logical_not(last))
            def _():
                copy_z(v).start()

                @pl.when(v == nr - 1)
                def _():
                    send_sh()

            @pl.when(last)
            def _():
                out_h(v).start()
                copy_ho(v).start()

            @pl.when(v + 2 < nr)
            def _():
                copy_y(v + 2).start()

        def w_words(v):
            def group(n):
                for k in range(GROUP):
                    w_tile(n * GROUP + k, v)
            each(ND // GROUP, group)

        def t3(v):
            copy_z(v).wait_recv()
            h_t[words_at(v), :] = h_bf[v].T

            @pl.when(v < nr - 1)
            def _():
                w_words(v)

        def update_s():
            for g in range(vh // LANES):
                at = slice(g * LANES, (g + 1) * LANES)
                fresh = h_s[:, at] * a_s[:, at] / sw_col[...]
                h_s[:, at] = fresh
                sh_acc[...] += fresh
            h_bf[nr, :, shared(y)] = h_s[...].astype(BF16)

            @pl.when(jnp.logical_not(last))
            def _():
                copy_zs().start()

            @pl.when(last)
            def _():
                out_s().start()
                copy_hs().start()

        def h_step(it):
            @pl.when(it < nr)
            def _():
                t1(it)

            @pl.when(it == jnp.where(sweep == 0, 1, 0))
            def _():
                each(ND, lambda d: copy_u(d).wait_recv())
                for step in range(1, cols):
                    copy_b(step).start()

                @pl.when(last)
                def _():
                    each(ND, give)

            @pl.when(it == S_OTHER)
            def _():
                @pl.when(sweep == 0)
                def _():
                    copy_c().wait()
                for step in range(1, cols):
                    copy_b(step).wait()
                each(ND // 2, s_other)

            @pl.when(it == S_OTHER + 1)
            def _():
                each(ND // 2, lambda d: s_other(d + ND // 2))
                update_s()

            @pl.when(jnp.logical_and(it == nr - 1, jnp.logical_not(last)))
            def _():
                copy_zs().wait_recv()
                h_t[words_at(nr), :] = h_bf[nr].T
                w_words(nr)

            @pl.when(jnp.logical_and(it >= 1, jnp.logical_not(last)))
            def _():
                t3(it - 1)

        @pl.when(sweep == 0)
        def _():
            each(ND, lambda d: copy_u(d).start())

        each(ND, s_own)
        each(nr + 1, h_step)

        def h_sent(v):
            copy_y(v).wait_send()

            @pl.when(jnp.logical_not(last))
            def _():
                copy_z(v).wait_send()

        each(nr, h_sent)
        each(ND, lambda d: copy_u(d).wait_send())

        @pl.when(jnp.logical_not(last))
        def _():
            copy_zs().wait_send()
        return carry

    lax.fori_loop(0, SWEEPS, sweep_body, 0)

    def finish_w(d):
        out_w(d).wait()
        for step in range(1, cols):
            copy_wo(d, step).wait()

    def finish_h(v):
        out_h(v).wait()
        copy_ho(v).wait()

    each(ND, finish_w)
    each(nr, finish_h)
    out_s().wait()
    copy_hs().wait()


def solution(mesh):
    rows, cols = mesh.shape["row"], mesh.shape["col"]
    n_dev = rows * cols

    def local(c_blk, w_loc, h_loc):
        docs, words = c_blk.shape
        topics = w_loc.shape[1]
        vmem = pltpu.VMEM
        dma = pltpu.SemaphoreType.DMA
        chunk = words // NV
        scratch = [
            vmem((docs, words), BF16),
            vmem((docs, topics), BF16),
            vmem((topics, docs // ND), BF16),
            vmem((NV, topics, chunk), BF16),
            vmem((words, topics), BF16),
            vmem((docs // 4, topics), F32),
            vmem((NV - 1, topics // 2, chunk), F32),
            vmem((docs, topics), F32),
            vmem((NV, topics, chunk), F32),
            vmem((docs // 2, topics), F32),
            vmem((docs // 4, topics), F32),
            vmem((NV - 1, topics // 2, chunk), F32),
            vmem((8, topics), F32),
            vmem((n_dev, 8, topics), F32),
            vmem((topics, LANES), F32),
            vmem((topics, LANES), F32),
            vmem((8, topics), F32),
            vmem((n_dev, 8, topics), F32),
            vmem((8, topics), F32),
            vmem((docs, chunk // 2), BF16),
            vmem((ND, 4, docs // ND // 4, topics), BF16),
            vmem((topics, chunk // 2), F32),
            vmem((topics, chunk // 2), F32),
        ]
        sizes = [1, 1, ND, ND, cols - 1, cols - 1, 4, 1, ND, NV, ND]
        sizes += [ND] * 10 + [NV] * 4 + [n_dev - 1] * 4 + [ND * (cols - 1)] * 2 + [NV] * 2 + [ND, NV]
        scratch += [dma((size,)) for size in sizes]
        any_space = pl.BlockSpec(memory_space=pl.ANY)
        return pl.pallas_call(
            functools.partial(kernel, rows, cols),
            out_shape=(jax.ShapeDtypeStruct(w_loc.shape, F32), jax.ShapeDtypeStruct(h_loc.shape, F32)),
            in_specs=[any_space] * 3,
            out_specs=(any_space, any_space),
            scratch_shapes=scratch,
            compiler_params=pltpu.CompilerParams(
                collective_id=0, has_side_effects=True, vmem_limit_bytes=67_043_328),
            name="nmf",
        )(c_blk, w_loc, h_loc)

    spec_c = P(("part", "row"), "col")
    spec_w = P(("part", "row"), None)
    spec_h = P(None, ("part", "col"))
    return jax.shard_map(local, mesh=mesh, in_specs=(spec_c, spec_w, spec_h), out_specs=(spec_w, spec_h), check_vma=False)
```

```python
import functools

import jax
import jax.numpy as jnp
from jax import lax
from jax.experimental import pallas as pl
from jax.experimental.pallas import tpu as pltpu
from jax.sharding import PartitionSpec as P

SWEEPS = 4
EPS = 1e-6
ND = 8
NV = 8
GROUP = 4
S_OTHER = 3
LAG1, LAG2, LAG3, LAG5 = 2, 4, 5, 6
LANES = 128
MESH = pl.DeviceIdType.MESH
F32 = jnp.float32
BF16 = jnp.bfloat16


def kernel(
    rows, cols, c_hbm, w_hbm, h_hbm, w_out, h_out,
    c_v, w_bf, w_t, h_bf, h_t, w_f, h_f, a_w, a_h, r_a, r_x, r_y,
    sw_acc, sw_slots, sw_col, sh_acc, sh_part, sh_slots, sh_row,
    c_two, w_two, a_s, h_s, c_send, c_recv, u_send, u_recv, b_send, b_recv, s_sems, os_sem,
    a_o, r_o, o_sems,
    w_sem, h_sem, c_sem,
    a_send, a_recv, x_send, x_recv, g_send, g_recv, p_send, p_recv, q_send, q_recv,
    y_send, y_recv, z_send, z_recv, sw_send, sw_recv, sh_send, sh_recv,
    wo_send, wo_recv, ho_send, ho_recv, ow_sem, oh_sem,
):
    docs, words = c_v.shape
    topics = w_bf.shape[1]
    dt, vt, kh = docs // ND, words // NV, topics // 2
    half, quarter = dt // 2, dt // 4
    nr, vh = NV - 1, vt // 2
    n_dev = rows * cols
    y, i = lax.axis_index("row"), lax.axis_index("col")
    x, core = i // 2, i % 2
    me = y * cols + i
    partner = {"col": x * 2 + (1 - core)}
    across = {"col": (1 - x) * 2 + core}
    above = {"row": 1 - y}

    def peer(step):
        other = (me + step) % n_dev
        return {"row": other // cols, "col": other % cols}

    def rows_at(start, size):
        return pl.ds(pl.multiple_of(start, size), size)

    def remote(src, dst, send, recv, device):
        return pltpu.make_async_remote_copy(
            src_ref=src, dst_ref=dst, send_sem=send, recv_sem=recv, device_id=device, device_id_type=MESH)

    def mine(d):
        return rows_at(d * dt + core * half + x * quarter, quarter)

    def theirs(d):
        return rows_at(d * dt + core * half + (1 - x) * quarter, quarter)

    def copy_a(d):
        return remote(a_w.at[rows_at(d * dt + (1 - core) * half, half)], r_a.at[rows_at(d * half, half)],
                      a_send.at[d], a_recv.at[d], partner)

    def copy_x(d):
        return remote(a_w.at[theirs(d)], r_x.at[rows_at(d * quarter, quarter)], x_send.at[d], x_recv.at[d], across)

    def copy_g(d):
        return remote(w_bf.at[mine(d)], w_bf.at[mine(d)], g_send.at[d], g_recv.at[d], across)

    def copy_p(d):
        return remote(w_bf.at[mine(d)], w_bf.at[mine(d)], p_send.at[d], p_recv.at[d], partner)

    def copy_q(d):
        return remote(w_bf.at[theirs(d)], w_bf.at[theirs(d)], q_send.at[d], q_recv.at[d], partner)

    own_k, other_k = rows_at(y * kh, kh), rows_at((1 - y) * kh, kh)

    def words_at(v):
        return rows_at(v * vt, vt)

    def copy_y(v):
        return remote(a_h.at[v, other_k], r_y.at[v], y_send.at[v], y_recv.at[v], above)

    def copy_z(v):
        return remote(h_bf.at[v, own_k], h_bf.at[v, own_k], z_send.at[v], z_recv.at[v], above)

    def shared(side):
        return rows_at(side * vh, vh)

    def whole(side):
        return rows_at(nr * vt + side * vh, vh)

    def copy_c():
        return remote(c_hbm.at[:, whole(1 - y)], c_two, c_send.at[0], c_recv.at[0], above)

    def copy_o():
        return remote(a_o, r_o, o_sems.at[0], o_sems.at[1], above)

    def copy_u(d):
        return remote(w_bf.at[mine(d)], w_two.at[d, core * 2 + x], u_send.at[d], u_recv.at[d], above)

    def copy_b(step):
        strip = w_two.at[:, core * 2 + x]
        return remote(strip, strip, b_send.at[step - 1], b_recv.at[step - 1], {"col": (i + step) % cols})

    def copy_zs():
        return remote(h_bf.at[nr, :, shared(y)], h_bf.at[nr, :, shared(y)], s_sems.at[0], s_sems.at[1], above)

    def copy_hs():
        return remote(h_s, h_out.at[:, whole(y)], s_sems.at[2], s_sems.at[3], above)

    def out_s():
        return pltpu.make_async_copy(h_s, h_out.at[:, whole(y)], os_sem.at[0])

    def copy_sw(step):
        return remote(sw_acc, sw_slots.at[me], sw_send.at[step - 1], sw_recv.at[step - 1], peer(step))

    def copy_sh(step):
        return remote(sh_part, sh_slots.at[me], sh_send.at[step - 1], sh_recv.at[step - 1], peer(step))

    def copy_wo(d, step):
        k = d * (cols - 1) + step - 1
        return remote(w_f.at[rows_at(d * quarter, quarter)], w_out.at[mine(d)], wo_send.at[k], wo_recv.at[k],
                      {"col": (i + step) % cols})

    def copy_ho(v):
        return remote(h_f.at[v], h_out.at[own_k, words_at(v)], ho_send.at[v], ho_recv.at[v], above)

    def out_w(d):
        return pltpu.make_async_copy(w_f.at[rows_at(d * quarter, quarter)], w_out.at[mine(d)], ow_sem.at[d])

    def out_h(v):
        return pltpu.make_async_copy(h_f.at[v], h_out.at[own_k, words_at(v)], oh_sem.at[v])

    def load_c(d):
        return pltpu.make_async_copy(c_hbm.at[rows_at(d * dt, dt)], c_v.at[rows_at(d * dt, dt)], c_sem.at[d])

    def each(count, body):
        def step(n, carry):
            body(n)
            return carry
        lax.fori_loop(0, count, step, 0)

    def ratio(d, v):
        z = jnp.dot(w_bf[rows_at(d * dt, dt), :], h_bf[v], preferred_element_type=F32)
        return (c_v[rows_at(d * dt, dt), words_at(v)].astype(F32) / (z + EPS)).astype(BF16)

    def select(first, held):
        if isinstance(first, bool):
            return jnp.zeros_like(held) if first else held
        return jnp.where(first, 0.0, held)

    def w_tile(d, v):
        part = jnp.dot(ratio(d, v), h_t[words_at(v), :], preferred_element_type=F32)
        held = a_w[rows_at(d * dt, dt), :]
        a_w[rows_at(d * dt, dt), :] = select(v == 0, held) + part

    def h_tile(d, v):
        part = jnp.dot(w_t[...], ratio(d, v), preferred_element_type=F32)
        held = a_h[v]
        a_h[v] = select(d == 0, held) + part

    def s_tile(total, rows_bf, counts, h_half, first):
        z = jnp.dot(rows_bf, h_half, preferred_element_type=F32)
        q = (counts.astype(F32) / (z + EPS)).astype(BF16)
        part = jnp.dot(rows_bf.T, q, preferred_element_type=F32)
        total[...] = jnp.where(first, 0.0, total[...]) + part

    def s_own(d):
        at = rows_at(d * dt, dt)
        s_tile(a_s, w_bf[at, :], c_v[at, whole(y)], h_bf[nr, :, shared(y)], d == 0)

    def s_cross(d):
        at = rows_at(d * dt, dt)
        s_tile(a_o, w_bf[at, :], c_v[at, whole(1 - y)], h_bf[nr, :, shared(1 - y)], d == 0)

    def s_other(d):
        s_tile(a_s, w_two[d].reshape(dt, topics), c_two[rows_at(d * dt, dt), :], h_bf[nr, :, shared(y)], False)

    def fold_lanes(block):
        total = block[:, :LANES]
        for g in range(1, block.shape[1] // LANES):
            total = total + block[:, g * LANES:(g + 1) * LANES]
        return total

    def send_sh():
        for r in range(rows):
            at = slice(r * kh, (r + 1) * kh)
            sh_part[:, at] = jnp.sum(sh_acc[at, :].T.reshape(LANES // 8, 8, kh), axis=0)
        sh_slots[me] = sh_part[...]
        for step in range(1, n_dev):
            copy_sh(step).start()

    def take_sh():
        for step in range(1, n_dev):
            copy_sh(step).wait()
        total = sh_slots[0]
        for n in range(1, n_dev):
            total = total + sh_slots[n]
        sh_row[...] = jnp.broadcast_to(jnp.sum(total, axis=0, keepdims=True), (8, topics))

    def send_sw():
        sw_slots[me] = sw_acc[...]
        for step in range(1, n_dev):
            copy_sw(step).start()

    def take_sw():
        for step in range(1, n_dev):
            copy_sw(step).wait()
        total = sw_slots[0]
        for n in range(1, n_dev):
            total = total + sw_slots[n]
        total = jnp.sum(total, axis=0, keepdims=True)
        for r in range(rows):
            at = slice(r * kh, (r + 1) * kh)
            sw_col[at, :] = jnp.broadcast_to(total[:, at], (LANES, kh)).T

    def load_h(v):
        return pltpu.make_async_copy(h_hbm.at[:, words_at(v)], a_h.at[v], h_sem.at[v])

    def load_w(d):
        return pltpu.make_async_copy(w_hbm.at[rows_at(d * dt, dt)], a_w.at[rows_at(d * dt, dt)], w_sem.at[d])

    barrier = pltpu.get_barrier_semaphore()
    for step in range(1, n_dev):
        pl.semaphore_signal(barrier, inc=1, device_id=peer(step), device_id_type=MESH)
    each(NV, lambda v: load_h(v).start())
    load_w(0).start()
    load_c(0).start()
    sh_acc[...] = jnp.zeros_like(sh_acc)

    def start_h(v):
        load_h(v).wait()
        h_bf[v] = a_h[v].astype(BF16)
        h_t[words_at(v), :] = h_bf[v].T

        @pl.when(v < nr)
        def _():
            own = a_h[v, own_k]
            h_f[v] = own
            sh_acc[own_k, :] += fold_lanes(own)

        @pl.when(v == nr)
        def _():
            own = a_h[nr, :, shared(y)]
            h_s[...] = own
            sh_acc[...] += fold_lanes(own)

        @pl.when(v + 1 < ND)
        def _():
            load_w(v + 1).start()
            load_c(v + 1).start()

    each(NV, start_h)
    pl.semaphore_wait(barrier, n_dev - 1)
    send_sh()
    copy_c().start()

    def start_w(d):
        load_w(d).wait()
        w_bf[rows_at(d * dt, dt), :] = a_w[rows_at(d * dt, dt), :].astype(BF16)
        w_f[rows_at(d * quarter, quarter), :] = a_w[mine(d), :]
        load_c(d).wait()

    def sweep_body(sweep, carry):
        last = sweep == SWEEPS - 1

        def s0(d):
            @pl.when(sweep == 0)
            def _():
                start_w(d)
                for v in range(NV):
                    w_tile(d, v)

            @pl.when(sweep > 0)
            def _():
                w_tile(d, nr - 1)
            copy_a(d).start()

        def s1(d):
            copy_a(d).wait_recv()
            own = rows_at(d * dt + core * half, half)
            a_w[own, :] += r_a[rows_at(d * half, half), :]
            copy_x(d).start()

        def s2(d):
            @pl.when(d == 0)
            def _():
                take_sh()
                sw_acc[...] = jnp.zeros_like(sw_acc)
            copy_x(d).wait_recv()
            own = rows_at(d * quarter, quarter)
            fresh = w_f[own, :] * (a_w[mine(d), :] + r_x[own, :]) / sh_row[0:1, :]
            w_f[own, :] = fresh
            w_bf[mine(d), :] = fresh.astype(BF16)
            copy_g(d).start()
            copy_p(d).start()

            @pl.when(sweep > 0)
            def _():
                copy_u(d).start()
            sw_acc[...] += jnp.sum(fresh.reshape(quarter // 8, 8, topics), axis=0)

            @pl.when(d == ND - 1)
            def _():
                send_sw()

        def s3(d):
            copy_g(d).wait_recv()
            copy_q(d).start()

        def s5(d):
            copy_p(d).wait_recv()
            copy_q(d).wait_recv()
            w_t[...] = w_bf[rows_at(d * dt, dt), :].T

            @pl.when(d < ND - 1)
            def _():
                for v in range(nr):
                    h_tile(d, v)

            @pl.when(d == ND - 1)
            def _():
                h_tile(d, 0)
                h_tile(d, 1)
                copy_y(0).start()
                copy_y(1).start()
                for v in range(2, nr):
                    h_tile(d, v)

        def stage(it, lag, body):
            @pl.when(jnp.logical_and(it >= lag, it < lag + ND))
            def _():
                body(it - lag)

        def w_step(it):
            for lag, body in ((LAG2, s2), (LAG1, s1), (0, s0), (LAG3, s3), (LAG5, s5)):
                stage(it, lag, body)

        each(ND + LAG5, w_step)

        def w_sent(d):
            copy_a(d).wait_send()
            copy_x(d).wait_send()
            copy_g(d).wait_send()
            copy_p(d).wait_send()
            copy_q(d).wait_send()

        each(ND, w_sent)

        def give(d):
            out_w(d).start()
            for step in range(1, cols):
                copy_wo(d, step).start()

        def t1(v):
            @pl.when(v == 0)
            def _():
                take_sw()
                sh_acc[...] = jnp.zeros_like(sh_acc)
            copy_y(v).wait_recv()
            for g in range(vt // LANES):
                at = slice(g * LANES, (g + 1) * LANES)
                fresh = h_f[v, :, at] * (a_h[v, own_k, at] + r_y[v, :, at]) / sw_col[own_k, :]
                h_f[v, :, at] = fresh
                h_bf[v, own_k, at] = fresh.astype(BF16)
                sh_acc[own_k, :] += fresh

            @pl.when(jnp.logical_not(last))
            def _():
                copy_z(v).start()

                @pl.when(v == nr - 1)
                def _():
                    send_sh()

            @pl.when(last)
            def _():
                out_h(v).start()
                copy_ho(v).start()

            @pl.when(v + 2 < nr)
            def _():
                copy_y(v + 2).start()

        def w_words(v):
            def group(n):
                for k in range(GROUP):
                    w_tile(n * GROUP + k, v)
            each(ND // GROUP, group)

        def t3(v):
            copy_z(v).wait_recv()
            h_t[words_at(v), :] = h_bf[v].T

            @pl.when(v < nr - 1)
            def _():
                w_words(v)

        def update_s():
            for g in range(vh // LANES):
                at = slice(g * LANES, (g + 1) * LANES)
                fresh = h_s[:, at] * a_s[:, at] / sw_col[...]
                h_s[:, at] = fresh
                sh_acc[...] += fresh
            h_bf[nr, :, shared(y)] = h_s[...].astype(BF16)

            @pl.when(jnp.logical_not(last))
            def _():
                copy_zs().start()

            @pl.when(last)
            def _():
                out_s().start()
                copy_hs().start()

        def h_step(it):
            @pl.when(it < nr)
            def _():
                t1(it)

            @pl.when(jnp.logical_and(it == 0, sweep > 0))
            def _():
                each(ND, lambda d: copy_u(d).wait_recv())
                for step in range(1, cols):
                    copy_b(step).start()

                @pl.when(last)
                def _():
                    each(ND, give)

            @pl.when(jnp.logical_and(it == S_OTHER, sweep == 0))
            def _():
                copy_o().wait()
                a_s[...] += r_o[...]

            @pl.when(jnp.logical_and(it == S_OTHER, sweep > 0))
            def _():
                @pl.when(sweep == 1)
                def _():
                    copy_c().wait()
                for step in range(1, cols):
                    copy_b(step).wait()
                each(ND // 2, s_other)

            @pl.when(it == S_OTHER + 1)
            def _():
                @pl.when(sweep > 0)
                def _():
                    each(ND // 2, lambda d: s_other(d + ND // 2))
                update_s()

            @pl.when(jnp.logical_and(it == nr - 1, jnp.logical_not(last)))
            def _():
                copy_zs().wait_recv()
                h_t[words_at(nr), :] = h_bf[nr].T
                w_words(nr)

            @pl.when(jnp.logical_and(it >= 1, jnp.logical_not(last)))
            def _():
                t3(it - 1)

        @pl.when(sweep == 0)
        def _():
            each(ND, s_cross)
            copy_o().start()

        each(ND, s_own)
        each(nr + 1, h_step)

        def h_sent(v):
            copy_y(v).wait_send()

            @pl.when(jnp.logical_not(last))
            def _():
                copy_z(v).wait_send()

        each(nr, h_sent)
        @pl.when(sweep > 0)
        def _():
            each(ND, lambda d: copy_u(d).wait_send())

        @pl.when(jnp.logical_not(last))
        def _():
            copy_zs().wait_send()
        return carry

    lax.fori_loop(0, SWEEPS, sweep_body, 0)

    def finish_w(d):
        out_w(d).wait()
        for step in range(1, cols):
            copy_wo(d, step).wait()

    def finish_h(v):
        out_h(v).wait()
        copy_ho(v).wait()

    each(ND, finish_w)
    each(nr, finish_h)
    out_s().wait()
    copy_hs().wait()


def solution(mesh):
    rows, cols = mesh.shape["row"], mesh.shape["col"]
    n_dev = rows * cols

    def local(c_blk, w_loc, h_loc):
        docs, words = c_blk.shape
        topics = w_loc.shape[1]
        vmem = pltpu.VMEM
        dma = pltpu.SemaphoreType.DMA
        chunk = words // NV
        scratch = [
            vmem((docs, words), BF16),
            vmem((docs, topics), BF16),
            vmem((topics, docs // ND), BF16),
            vmem((NV, topics, chunk), BF16),
            vmem((words, topics), BF16),
            vmem((docs // 4, topics), F32),
            vmem((NV - 1, topics // 2, chunk), F32),
            vmem((docs, topics), F32),
            vmem((NV, topics, chunk), F32),
            vmem((docs // 2, topics), F32),
            vmem((docs // 4, topics), F32),
            vmem((NV - 1, topics // 2, chunk), F32),
            vmem((8, topics), F32),
            vmem((n_dev, 8, topics), F32),
            vmem((topics, LANES), F32),
            vmem((topics, LANES), F32),
            vmem((8, topics), F32),
            vmem((n_dev, 8, topics), F32),
            vmem((8, topics), F32),
            vmem((docs, chunk // 2), BF16),
            vmem((ND, 4, docs // ND // 4, topics), BF16),
            vmem((topics, chunk // 2), F32),
            vmem((topics, chunk // 2), F32),
        ]
        sizes = [1, 1, ND, ND, cols - 1, cols - 1, 4, 1, ND, NV, ND]
        sizes += [ND] * 10 + [NV] * 4 + [n_dev - 1] * 4 + [ND * (cols - 1)] * 2 + [NV] * 2 + [ND, NV]
        scratch += [dma((size,)) for size in sizes]
        extra = [vmem((topics, chunk // 2), F32), vmem((topics, chunk // 2), F32), dma((2,))]
        scratch[31:31] = extra
        any_space = pl.BlockSpec(memory_space=pl.ANY)
        return pl.pallas_call(
            functools.partial(kernel, rows, cols),
            out_shape=(jax.ShapeDtypeStruct(w_loc.shape, F32), jax.ShapeDtypeStruct(h_loc.shape, F32)),
            in_specs=[any_space] * 3,
            out_specs=(any_space, any_space),
            scratch_shapes=scratch,
            compiler_params=pltpu.CompilerParams(
                collective_id=0, has_side_effects=True, vmem_limit_bytes=67_043_328),
            name="nmf",
        )(c_blk, w_loc, h_loc)

    spec_c = P(("part", "row"), "col")
    spec_w = P(("part", "row"), None)
    spec_h = P(None, ("part", "col"))
    return jax.shard_map(local, mesh=mesh, in_specs=(spec_c, spec_w, spec_h), out_specs=(spec_w, spec_h), check_vma=False)
```

```python
import functools

import jax
import jax.numpy as jnp
from jax import lax
from jax.experimental import pallas as pl
from jax.experimental.pallas import tpu as pltpu
from jax.sharding import PartitionSpec as P

SWEEPS = 4
EPS = 1e-6
ND = 8
NV = 8
GROUP = 4
NS = 2
S_OTHER = 3
LAG1, LAG2, LAG3, LAG5 = 2, 4, 5, 6
LANES = 128
MESH = pl.DeviceIdType.MESH
F32 = jnp.float32
BF16 = jnp.bfloat16


def kernel(
    rows, cols, c_hbm, w_hbm, h_hbm, w_out, h_out,
    c_v, w_bf, w_t, h_bf, h_t, w_f, h_f, a_w, a_h, r_a, r_x, r_y,
    sw_acc, sw_slots, sw_col, sh_acc, sh_part, sh_slots, sh_row,
    c_two, w_two, a_s, h_s, c_send, c_recv, u_send, u_recv, b_send, b_recv, s_sems, os_sem,
    a_o, r_o, o_sems,
    w_sem, h_sem, c_sem,
    a_send, a_recv, x_send, x_recv, g_send, g_recv, p_send, p_recv, q_send, q_recv,
    y_send, y_recv, z_send, z_recv, sw_send, sw_recv, sh_send, sh_recv,
    wo_send, wo_recv, ho_send, ho_recv, ow_sem, oh_sem,
):
    docs, words = c_v.shape
    topics = w_bf.shape[1]
    dt, vt, kh = docs // ND, words // NV, topics // 2
    half, quarter = dt // 2, dt // 4
    nr, vh = NV - NS, vt // 2
    n_dev = rows * cols
    y, i = lax.axis_index("row"), lax.axis_index("col")
    x, core = i // 2, i % 2
    me = y * cols + i
    partner = {"col": x * 2 + (1 - core)}
    across = {"col": (1 - x) * 2 + core}
    above = {"row": 1 - y}

    def peer(step):
        other = (me + step) % n_dev
        return {"row": other // cols, "col": other % cols}

    def rows_at(start, size):
        return pl.ds(pl.multiple_of(start, size), size)

    def remote(src, dst, send, recv, device):
        return pltpu.make_async_remote_copy(
            src_ref=src, dst_ref=dst, send_sem=send, recv_sem=recv, device_id=device, device_id_type=MESH)

    def mine(d):
        return rows_at(d * dt + core * half + x * quarter, quarter)

    def theirs(d):
        return rows_at(d * dt + core * half + (1 - x) * quarter, quarter)

    def copy_a(d):
        return remote(a_w.at[rows_at(d * dt + (1 - core) * half, half)], r_a.at[rows_at(d * half, half)],
                      a_send.at[d], a_recv.at[d], partner)

    def copy_x(d):
        return remote(a_w.at[theirs(d)], r_x.at[rows_at(d * quarter, quarter)], x_send.at[d], x_recv.at[d], across)

    def copy_g(d):
        return remote(w_bf.at[mine(d)], w_bf.at[mine(d)], g_send.at[d], g_recv.at[d], across)

    def copy_p(d):
        return remote(w_bf.at[mine(d)], w_bf.at[mine(d)], p_send.at[d], p_recv.at[d], partner)

    def copy_q(d):
        return remote(w_bf.at[theirs(d)], w_bf.at[theirs(d)], q_send.at[d], q_recv.at[d], partner)

    own_k, other_k = rows_at(y * kh, kh), rows_at((1 - y) * kh, kh)

    def words_at(v):
        return rows_at(v * vt, vt)

    def copy_y(v):
        return remote(a_h.at[v, other_k], r_y.at[v], y_send.at[v], y_recv.at[v], above)

    def copy_z(v):
        return remote(h_bf.at[v, own_k], h_bf.at[v, own_k], z_send.at[v], z_recv.at[v], above)

    def shared(side):
        return rows_at(side * vh, vh)

    def whole(k, side):
        return rows_at((NV - 1 - k) * vt + side * vh, vh)

    def copy_c(k, d):
        at = rows_at(d * dt, dt)
        return remote(c_hbm.at[at, whole(k, 1 - y)], c_two.at[k, at], c_send.at[k, d], c_recv.at[k, d], above)

    def copy_o(k):
        return remote(a_o.at[k], r_o.at[k], o_sems.at[k, 0], o_sems.at[k, 1], above)

    def copy_u(d):
        return remote(w_bf.at[mine(d)], w_two.at[d, core * 2 + x], u_send.at[d], u_recv.at[d], above)

    def copy_b(step):
        strip = w_two.at[:, core * 2 + x]
        return remote(strip, strip, b_send.at[step - 1], b_recv.at[step - 1], {"col": (i + step) % cols})

    def copy_zs(k):
        part = h_bf.at[NV - 1 - k, :, shared(y)]
        return remote(part, part, s_sems.at[k, 0], s_sems.at[k, 1], above)

    def copy_hs(k):
        return remote(h_s.at[k], h_out.at[:, whole(k, y)], s_sems.at[k, 2], s_sems.at[k, 3], above)

    def out_s(k):
        return pltpu.make_async_copy(h_s.at[k], h_out.at[:, whole(k, y)], os_sem.at[k])

    def copy_sw(step):
        return remote(sw_acc, sw_slots.at[me], sw_send.at[step - 1], sw_recv.at[step - 1], peer(step))

    def copy_sh(step):
        return remote(sh_part, sh_slots.at[me], sh_send.at[step - 1], sh_recv.at[step - 1], peer(step))

    def copy_wo(d, step):
        k = d * (cols - 1) + step - 1
        return remote(w_f.at[rows_at(d * quarter, quarter)], w_out.at[mine(d)], wo_send.at[k], wo_recv.at[k],
                      {"col": (i + step) % cols})

    def copy_ho(v):
        return remote(h_f.at[v], h_out.at[own_k, words_at(v)], ho_send.at[v], ho_recv.at[v], above)

    def out_w(d):
        return pltpu.make_async_copy(w_f.at[rows_at(d * quarter, quarter)], w_out.at[mine(d)], ow_sem.at[d])

    def out_h(v):
        return pltpu.make_async_copy(h_f.at[v], h_out.at[own_k, words_at(v)], oh_sem.at[v])

    def load_c(d):
        return pltpu.make_async_copy(c_hbm.at[rows_at(d * dt, dt)], c_v.at[rows_at(d * dt, dt)], c_sem.at[d])

    def each(count, body):
        def step(n, carry):
            body(n)
            return carry
        lax.fori_loop(0, count, step, 0)

    def ratio(d, v):
        z = jnp.dot(w_bf[rows_at(d * dt, dt), :], h_bf[v], preferred_element_type=F32)
        return (c_v[rows_at(d * dt, dt), words_at(v)].astype(F32) / (z + EPS)).astype(BF16)

    def select(first, held):
        if isinstance(first, bool):
            return jnp.zeros_like(held) if first else held
        return jnp.where(first, 0.0, held)

    def w_tile(d, v):
        part = jnp.dot(ratio(d, v), h_t[words_at(v), :], preferred_element_type=F32)
        held = a_w[rows_at(d * dt, dt), :]
        a_w[rows_at(d * dt, dt), :] = select(v == 0, held) + part

    def h_tile(d, v):
        part = jnp.dot(w_t[...], ratio(d, v), preferred_element_type=F32)
        held = a_h[v]
        a_h[v] = select(d == 0, held) + part

    def s_tile(total, rows_bf, counts, h_half, first):
        z = jnp.dot(rows_bf, h_half, preferred_element_type=F32)
        q = (counts.astype(F32) / (z + EPS)).astype(BF16)
        part = jnp.dot(rows_bf.T, q, preferred_element_type=F32)
        total[...] = jnp.where(first, 0.0, total[...]) + part

    def s_own(k, d):
        at = rows_at(d * dt, dt)
        s_tile(a_s.at[k], w_bf[at, :], c_v[at, whole(k, y)], h_bf[NV - 1 - k, :, shared(y)], d == 0)

    def s_cross(k, d):
        at = rows_at(d * dt, dt)
        s_tile(a_o.at[k], w_bf[at, :], c_v[at, whole(k, 1 - y)], h_bf[NV - 1 - k, :, shared(1 - y)], d == 0)

    def s_other(k, d):
        counts = c_two[k, rows_at(d * dt, dt), :]
        s_tile(a_s.at[k], w_two[d].reshape(dt, topics), counts, h_bf[NV - 1 - k, :, shared(y)], False)

    def fold_lanes(block):
        total = block[:, :LANES]
        for g in range(1, block.shape[1] // LANES):
            total = total + block[:, g * LANES:(g + 1) * LANES]
        return total

    def send_sh():
        for r in range(rows):
            at = slice(r * kh, (r + 1) * kh)
            sh_part[:, at] = jnp.sum(sh_acc[at, :].T.reshape(LANES // 8, 8, kh), axis=0)
        sh_slots[me] = sh_part[...]
        for step in range(1, n_dev):
            copy_sh(step).start()

    def take_sh():
        for step in range(1, n_dev):
            copy_sh(step).wait()
        total = sh_slots[0]
        for n in range(1, n_dev):
            total = total + sh_slots[n]
        sh_row[...] = jnp.broadcast_to(jnp.sum(total, axis=0, keepdims=True), (8, topics))

    def send_sw():
        sw_slots[me] = sw_acc[...]
        for step in range(1, n_dev):
            copy_sw(step).start()

    def take_sw():
        for step in range(1, n_dev):
            copy_sw(step).wait()
        total = sw_slots[0]
        for n in range(1, n_dev):
            total = total + sw_slots[n]
        total = jnp.sum(total, axis=0, keepdims=True)
        for r in range(rows):
            at = slice(r * kh, (r + 1) * kh)
            sw_col[at, :] = jnp.broadcast_to(total[:, at], (LANES, kh)).T

    def load_h(v):
        return pltpu.make_async_copy(h_hbm.at[:, words_at(v)], a_h.at[v], h_sem.at[v])

    def load_w(d):
        return pltpu.make_async_copy(w_hbm.at[rows_at(d * dt, dt)], a_w.at[rows_at(d * dt, dt)], w_sem.at[d])

    barrier = pltpu.get_barrier_semaphore()
    for step in range(1, n_dev):
        pl.semaphore_signal(barrier, inc=1, device_id=peer(step), device_id_type=MESH)
    each(NV, lambda v: load_h(v).start())
    load_w(0).start()
    load_c(0).start()
    sh_acc[...] = jnp.zeros_like(sh_acc)

    def start_h(v):
        load_h(v).wait()
        h_bf[v] = a_h[v].astype(BF16)
        h_t[words_at(v), :] = h_bf[v].T

        @pl.when(v < nr)
        def _():
            own = a_h[v, own_k]
            h_f[v] = own
            sh_acc[own_k, :] += fold_lanes(own)

        @pl.when(v >= nr)
        def _():
            own = a_h[v, :, shared(y)]
            h_s[NV - 1 - v] = own
            sh_acc[...] += fold_lanes(own)

        @pl.when(v + 1 < ND)
        def _():
            load_w(v + 1).start()
            load_c(v + 1).start()

    each(NV, start_h)
    pl.semaphore_wait(barrier, n_dev - 1)
    send_sh()
    each(ND, lambda d: copy_c(0, d).start())

    def start_w(d):
        load_w(d).wait()
        w_bf[rows_at(d * dt, dt), :] = a_w[rows_at(d * dt, dt), :].astype(BF16)
        w_f[rows_at(d * quarter, quarter), :] = a_w[mine(d), :]
        load_c(d).wait()

    def sweep_body(sweep, carry):
        last = sweep == SWEEPS - 1

        def s0(d):
            @pl.when(sweep == 0)
            def _():
                start_w(d)
                for v in range(NV):
                    w_tile(d, v)

            @pl.when(sweep > 0)
            def _():
                w_tile(d, nr - 1)
            copy_a(d).start()

        def s1(d):
            copy_a(d).wait_recv()
            own = rows_at(d * dt + core * half, half)
            a_w[own, :] += r_a[rows_at(d * half, half), :]
            copy_x(d).start()

        def s2(d):
            @pl.when(d == 0)
            def _():
                take_sh()
                sw_acc[...] = jnp.zeros_like(sw_acc)
            copy_x(d).wait_recv()
            own = rows_at(d * quarter, quarter)
            fresh = w_f[own, :] * (a_w[mine(d), :] + r_x[own, :]) / sh_row[0:1, :]
            w_f[own, :] = fresh
            w_bf[mine(d), :] = fresh.astype(BF16)
            copy_g(d).start()
            copy_p(d).start()

            @pl.when(sweep > 0)
            def _():
                copy_u(d).start()

            for k in range(1, NS):
                @pl.when(jnp.logical_and(jnp.logical_or(sweep == k, sweep == k + 1), d < ND // 2))
                def _(k=k):
                    copy_c(k, (sweep - k) * (ND // 2) + d).start()
            sw_acc[...] += jnp.sum(fresh.reshape(quarter // 8, 8, topics), axis=0)

            @pl.when(d == ND - 1)
            def _():
                send_sw()

        def s3(d):
            copy_g(d).wait_recv()
            copy_q(d).start()

        def s5(d):
            copy_p(d).wait_recv()
            copy_q(d).wait_recv()
            w_t[...] = w_bf[rows_at(d * dt, dt), :].T

            @pl.when(d < ND - 1)
            def _():
                for v in range(nr):
                    h_tile(d, v)

            @pl.when(d == ND - 1)
            def _():
                h_tile(d, 0)
                h_tile(d, 1)
                copy_y(0).start()
                copy_y(1).start()
                for v in range(2, nr):
                    h_tile(d, v)

        def stage(it, lag, body):
            @pl.when(jnp.logical_and(it >= lag, it < lag + ND))
            def _():
                body(it - lag)

        def w_step(it):
            for lag, body in ((LAG2, s2), (LAG1, s1), (0, s0), (LAG3, s3), (LAG5, s5)):
                stage(it, lag, body)

        each(ND + LAG5, w_step)

        def w_sent(d):
            copy_a(d).wait_send()
            copy_x(d).wait_send()
            copy_g(d).wait_send()
            copy_p(d).wait_send()
            copy_q(d).wait_send()

        each(ND, w_sent)

        def give(d):
            out_w(d).start()
            for step in range(1, cols):
                copy_wo(d, step).start()

        def t1(v):
            @pl.when(v == 0)
            def _():
                take_sw()
                sh_acc[...] = jnp.zeros_like(sh_acc)
            copy_y(v).wait_recv()
            for g in range(vt // LANES):
                at = slice(g * LANES, (g + 1) * LANES)
                fresh = h_f[v, :, at] * (a_h[v, own_k, at] + r_y[v, :, at]) / sw_col[own_k, :]
                h_f[v, :, at] = fresh
                h_bf[v, own_k, at] = fresh.astype(BF16)
                sh_acc[own_k, :] += fresh

            @pl.when(jnp.logical_not(last))
            def _():
                copy_z(v).start()

                @pl.when(v == nr - 1)
                def _():
                    send_sh()

            @pl.when(last)
            def _():
                out_h(v).start()
                copy_ho(v).start()

            @pl.when(v + 2 < nr)
            def _():
                copy_y(v + 2).start()

        def w_words(v):
            def group(n):
                for k in range(GROUP):
                    w_tile(n * GROUP + k, v)
            each(ND // GROUP, group)

        def t3(v):
            copy_z(v).wait_recv()
            h_t[words_at(v), :] = h_bf[v].T

            @pl.when(v < nr - 1)
            def _():
                w_words(v)

        def update_s(k):
            for g in range(vh // LANES):
                at = slice(g * LANES, (g + 1) * LANES)
                fresh = h_s[k, :, at] * a_s[k, :, at] / sw_col[...]
                h_s[k, :, at] = fresh
                sh_acc[...] += fresh
            h_bf[NV - 1 - k, :, shared(y)] = h_s[k].astype(BF16)

            @pl.when(jnp.logical_not(last))
            def _():
                copy_zs(k).start()

            @pl.when(last)
            def _():
                out_s(k).start()
                copy_hs(k).start()

        def whole_sum(k):
            @pl.when(sweep <= k)
            def _():
                copy_o(k).wait()
                a_s[k] += r_o[k]

            @pl.when(sweep > k)
            def _():
                @pl.when(sweep == k + 1)
                def _():
                    each(ND, lambda d: copy_c(k, d).wait())
                each(ND, lambda d: s_other(k, d))

        def h_step(it):
            @pl.when(it < nr)
            def _():
                t1(it)

            @pl.when(jnp.logical_and(it == 0, sweep > 0))
            def _():
                each(ND, lambda d: copy_u(d).wait_recv())
                for step in range(1, cols):
                    copy_b(step).start()

                @pl.when(last)
                def _():
                    each(ND, give)

            @pl.when(jnp.logical_and(it == S_OTHER, sweep > 0))
            def _():
                for step in range(1, cols):
                    copy_b(step).wait()

            for k in range(NS):
                @pl.when(it == S_OTHER + k)
                def _(k=k):
                    whole_sum(k)

            @pl.when(it == S_OTHER + NS - 1)
            def _():
                for k in range(NS):
                    update_s(k)

            @pl.when(jnp.logical_and(it >= 1, jnp.logical_not(last)))
            def _():
                t3(it - 1)

            @pl.when(jnp.logical_and(it == nr - 1, jnp.logical_not(last)))
            def _():
                for k in range(NS):
                    copy_zs(k).wait_recv()
                    h_t[words_at(NV - 1 - k), :] = h_bf[NV - 1 - k].T
                    w_words(NV - 1 - k)

        for k in range(NS):
            @pl.when(sweep <= k)
            def _(k=k):
                each(ND, lambda d: s_cross(k, d))
                copy_o(k).start()

        for k in range(NS):
            each(ND, lambda d: s_own(k, d))
        each(nr + 1, h_step)

        def h_sent(v):
            copy_y(v).wait_send()

            @pl.when(jnp.logical_not(last))
            def _():
                copy_z(v).wait_send()

        each(nr, h_sent)
        @pl.when(sweep > 0)
        def _():
            each(ND, lambda d: copy_u(d).wait_send())

        @pl.when(jnp.logical_not(last))
        def _():
            for k in range(NS):
                copy_zs(k).wait_send()
        return carry

    lax.fori_loop(0, SWEEPS, sweep_body, 0)

    def finish_w(d):
        out_w(d).wait()
        for step in range(1, cols):
            copy_wo(d, step).wait()

    def finish_h(v):
        out_h(v).wait()
        copy_ho(v).wait()

    each(ND, finish_w)
    each(nr, finish_h)
    for k in range(NS):
        out_s(k).wait()
        copy_hs(k).wait()


def solution(mesh):
    rows, cols = mesh.shape["row"], mesh.shape["col"]
    n_dev = rows * cols

    def local(c_blk, w_loc, h_loc):
        docs, words = c_blk.shape
        topics = w_loc.shape[1]
        vmem = pltpu.VMEM
        dma = pltpu.SemaphoreType.DMA
        chunk = words // NV
        scratch = [
            vmem((docs, words), BF16),
            vmem((docs, topics), BF16),
            vmem((topics, docs // ND), BF16),
            vmem((NV, topics, chunk), BF16),
            vmem((words, topics), BF16),
            vmem((docs // 4, topics), F32),
            vmem((NV - NS, topics // 2, chunk), F32),
            vmem((docs, topics), F32),
            vmem((NV, topics, chunk), F32),
            vmem((docs // 2, topics), F32),
            vmem((docs // 4, topics), F32),
            vmem((NV - NS, topics // 2, chunk), F32),
            vmem((8, topics), F32),
            vmem((n_dev, 8, topics), F32),
            vmem((topics, LANES), F32),
            vmem((topics, LANES), F32),
            vmem((8, topics), F32),
            vmem((n_dev, 8, topics), F32),
            vmem((8, topics), F32),
            vmem((NS, docs, chunk // 2), BF16),
            vmem((ND, 4, docs // ND // 4, topics), BF16),
            vmem((NS, topics, chunk // 2), F32),
            vmem((NS, topics, chunk // 2), F32),
        ]
        sizes = [(NS, ND)] * 2 + [ND, ND, cols - 1, cols - 1, (NS, 4), NS, ND, NV, ND]
        sizes += [ND] * 10 + [NV] * 4 + [n_dev - 1] * 4 + [ND * (cols - 1)] * 2 + [NV] * 2 + [ND, NV]
        scratch += [dma(size if isinstance(size, tuple) else (size,)) for size in sizes]
        extra = [vmem((NS, topics, chunk // 2), F32), vmem((NS, topics, chunk // 2), F32), dma((NS, 2))]
        scratch[31:31] = extra
        any_space = pl.BlockSpec(memory_space=pl.ANY)
        return pl.pallas_call(
            functools.partial(kernel, rows, cols),
            out_shape=(jax.ShapeDtypeStruct(w_loc.shape, F32), jax.ShapeDtypeStruct(h_loc.shape, F32)),
            in_specs=[any_space] * 3,
            out_specs=(any_space, any_space),
            scratch_shapes=scratch,
            compiler_params=pltpu.CompilerParams(
                collective_id=0, has_side_effects=True, vmem_limit_bytes=67_043_328),
            name="nmf",
        )(c_blk, w_loc, h_loc)

    spec_c = P(("part", "row"), "col")
    spec_w = P(("part", "row"), None)
    spec_h = P(None, ("part", "col"))
    return jax.shard_map(local, mesh=mesh, in_specs=(spec_c, spec_w, spec_h), out_specs=(spec_w, spec_h), check_vma=False)
```

```python
import functools

import jax
import jax.numpy as jnp
from jax import lax
from jax.experimental import pallas as pl
from jax.experimental.pallas import tpu as pltpu
from jax.sharding import PartitionSpec as P

SWEEPS = 4
EPS = 1e-6
ND = 8
NV = 8
GROUP = 4
NS = 3
PIECES = {1: (0, 6), 2: (6, 5), 3: (11, 5)}
S_OTHER = 3
LAG1, LAG2, LAG3, LAG5 = 2, 4, 5, 6
LANES = 128
MESH = pl.DeviceIdType.MESH
F32 = jnp.float32
BF16 = jnp.bfloat16


def kernel(
    rows, cols, c_hbm, w_hbm, h_hbm, w_out, h_out,
    c_v, w_bf, w_t, h_bf, h_t, w_f, h_f, a_w, a_h, r_a, r_x, r_y,
    sw_acc, sw_slots, sw_col, sh_acc, sh_part, sh_slots, sh_row,
    c_two, w_two, a_s, h_s, c_send, c_recv, u_send, u_recv, b_send, b_recv, s_sems, os_sem,
    a_o, r_o, o_sems,
    w_sem, h_sem, hs_sem, c_sem,
    a_send, a_recv, x_send, x_recv, g_send, g_recv, p_send, p_recv, q_send, q_recv,
    y_send, y_recv, z_send, z_recv, sw_send, sw_recv, sh_send, sh_recv,
    wo_send, wo_recv, ho_send, ho_recv, ow_sem, oh_sem,
):
    docs, words = c_v.shape
    topics = w_bf.shape[1]
    dt, vt, kh = docs // ND, words // NV, topics // 2
    half, quarter = dt // 2, dt // 4
    nr, vh = NV - NS, vt // 2
    n_dev = rows * cols
    y, i = lax.axis_index("row"), lax.axis_index("col")
    x, core = i // 2, i % 2
    me = y * cols + i
    partner = {"col": x * 2 + (1 - core)}
    across = {"col": (1 - x) * 2 + core}
    above = {"row": 1 - y}

    def peer(step):
        other = (me + step) % n_dev
        return {"row": other // cols, "col": other % cols}

    def rows_at(start, size):
        return pl.ds(pl.multiple_of(start, size), size)

    def remote(src, dst, send, recv, device):
        return pltpu.make_async_remote_copy(
            src_ref=src, dst_ref=dst, send_sem=send, recv_sem=recv, device_id=device, device_id_type=MESH)

    def mine(d):
        return rows_at(d * dt + core * half + x * quarter, quarter)

    def theirs(d):
        return rows_at(d * dt + core * half + (1 - x) * quarter, quarter)

    def copy_a(d):
        return remote(a_w.at[rows_at(d * dt + (1 - core) * half, half)], r_a.at[rows_at(d * half, half)],
                      a_send.at[d], a_recv.at[d], partner)

    def copy_x(d):
        return remote(a_w.at[theirs(d)], r_x.at[rows_at(d * quarter, quarter)], x_send.at[d], x_recv.at[d], across)

    def copy_g(d):
        return remote(w_bf.at[mine(d)], w_bf.at[mine(d)], g_send.at[d], g_recv.at[d], across)

    def copy_p(d):
        return remote(w_bf.at[mine(d)], w_bf.at[mine(d)], p_send.at[d], p_recv.at[d], partner)

    def copy_q(d):
        return remote(w_bf.at[theirs(d)], w_bf.at[theirs(d)], q_send.at[d], q_recv.at[d], partner)

    own_k, other_k = rows_at(y * kh, kh), rows_at((1 - y) * kh, kh)

    def words_at(v):
        return rows_at(v * vt, vt)

    def copy_y(v):
        return remote(a_h.at[v, other_k], r_y.at[v], y_send.at[v], y_recv.at[v], above)

    def copy_z(v):
        return remote(h_bf.at[v, own_k], h_bf.at[v, own_k], z_send.at[v], z_recv.at[v], above)

    def shared(side):
        return rows_at(side * vh, vh)

    def whole(k, side):
        return rows_at((NV - 1 - k) * vt + side * vh, vh)

    def copy_c(k, d):
        at = rows_at(d * dt, dt)
        return remote(c_hbm.at[at, whole(k, 1 - y)], c_two.at[k, at], c_send.at[k, d], c_recv.at[k, d], above)

    def copy_o(k):
        return remote(a_o.at[k], r_o.at[k], o_sems.at[k, 0], o_sems.at[k, 1], above)

    def copy_u(d):
        return remote(w_bf.at[mine(d)], w_two.at[d, core * 2 + x], u_send.at[d], u_recv.at[d], above)

    def copy_b(step):
        strip = w_two.at[:, core * 2 + x]
        return remote(strip, strip, b_send.at[step - 1], b_recv.at[step - 1], {"col": (i + step) % cols})

    def copy_zs(k):
        part = h_bf.at[NV - 1 - k, :, shared(y)]
        return remote(part, part, s_sems.at[k, 0], s_sems.at[k, 1], above)

    def copy_hs(k):
        return remote(h_s.at[k], h_out.at[:, whole(k, y)], s_sems.at[k, 2], s_sems.at[k, 3], above)

    def out_s(k):
        return pltpu.make_async_copy(h_s.at[k], h_out.at[:, whole(k, y)], os_sem.at[k])

    def copy_sw(step):
        return remote(sw_acc, sw_slots.at[me], sw_send.at[step - 1], sw_recv.at[step - 1], peer(step))

    def copy_sh(step):
        return remote(sh_part, sh_slots.at[me], sh_send.at[step - 1], sh_recv.at[step - 1], peer(step))

    def copy_wo(d, step):
        k = d * (cols - 1) + step - 1
        return remote(w_f.at[rows_at(d * quarter, quarter)], w_out.at[mine(d)], wo_send.at[k], wo_recv.at[k],
                      {"col": (i + step) % cols})

    def copy_ho(v):
        return remote(h_f.at[v], h_out.at[own_k, words_at(v)], ho_send.at[v], ho_recv.at[v], above)

    def out_w(d):
        return pltpu.make_async_copy(w_f.at[rows_at(d * quarter, quarter)], w_out.at[mine(d)], ow_sem.at[d])

    def out_h(v):
        return pltpu.make_async_copy(h_f.at[v], h_out.at[own_k, words_at(v)], oh_sem.at[v])

    def load_c(d):
        return pltpu.make_async_copy(c_hbm.at[rows_at(d * dt, dt)], c_v.at[rows_at(d * dt, dt)], c_sem.at[d])

    def each(count, body):
        def step(n, carry):
            body(n)
            return carry
        lax.fori_loop(0, count, step, 0)

    def ratio(d, v):
        z = jnp.dot(w_bf[rows_at(d * dt, dt), :], h_bf[v], preferred_element_type=F32)
        return (c_v[rows_at(d * dt, dt), words_at(v)].astype(F32) / (z + EPS)).astype(BF16)

    def select(first, held):
        if isinstance(first, bool):
            return jnp.zeros_like(held) if first else held
        return jnp.where(first, 0.0, held)

    def w_tile(d, v):
        part = jnp.dot(ratio(d, v), h_t[words_at(v), :], preferred_element_type=F32)
        held = a_w[rows_at(d * dt, dt), :]
        a_w[rows_at(d * dt, dt), :] = select(v == 0, held) + part

    def h_tile(d, v):
        part = jnp.dot(w_t[...], ratio(d, v), preferred_element_type=F32)
        held = a_h[v]
        a_h[v] = select(d == 0, held) + part

    def s_tile(total, rows_bf, counts, h_half, first):
        z = jnp.dot(rows_bf, h_half, preferred_element_type=F32)
        q = (counts.astype(F32) / (z + EPS)).astype(BF16)
        part = jnp.dot(rows_bf.T, q, preferred_element_type=F32)
        total[...] = jnp.where(first, 0.0, total[...]) + part

    def s_own(k, d):
        at = rows_at(d * dt, dt)
        s_tile(a_s.at[k], w_bf[at, :], c_v[at, whole(k, y)], h_bf[NV - 1 - k, :, shared(y)], d == 0)

    def s_cross(k, d):
        at = rows_at(d * dt, dt)
        s_tile(a_o.at[k], w_bf[at, :], c_v[at, whole(k, 1 - y)], h_bf[NV - 1 - k, :, shared(1 - y)], d == 0)

    def s_other(k, d):
        counts = c_two[k, rows_at(d * dt, dt), :]
        s_tile(a_s.at[k], w_two[d].reshape(dt, topics), counts, h_bf[NV - 1 - k, :, shared(y)], False)

    def fold_lanes(block):
        total = block[:, :LANES]
        for g in range(1, block.shape[1] // LANES):
            total = total + block[:, g * LANES:(g + 1) * LANES]
        return total

    def send_sh():
        for r in range(rows):
            at = slice(r * kh, (r + 1) * kh)
            sh_part[:, at] = jnp.sum(sh_acc[at, :].T.reshape(LANES // 8, 8, kh), axis=0)
        sh_slots[me] = sh_part[...]
        for step in range(1, n_dev):
            copy_sh(step).start()

    def take_sh():
        for step in range(1, n_dev):
            copy_sh(step).wait()
        total = sh_slots[0]
        for n in range(1, n_dev):
            total = total + sh_slots[n]
        sh_row[...] = jnp.broadcast_to(jnp.sum(total, axis=0, keepdims=True), (8, topics))

    def send_sw():
        sw_slots[me] = sw_acc[...]
        for step in range(1, n_dev):
            copy_sw(step).start()

    def take_sw():
        for step in range(1, n_dev):
            copy_sw(step).wait()
        total = sw_slots[0]
        for n in range(1, n_dev):
            total = total + sw_slots[n]
        total = jnp.sum(total, axis=0, keepdims=True)
        for r in range(rows):
            at = slice(r * kh, (r + 1) * kh)
            sw_col[at, :] = jnp.broadcast_to(total[:, at], (LANES, kh)).T

    def load_h(v):
        return pltpu.make_async_copy(h_hbm.at[:, words_at(v)], a_h.at[v], h_sem.at[v])

    def load_s(k, side):
        half_h = (a_o, r_o)[side].at[k]
        return pltpu.make_async_copy(h_hbm.at[:, whole(k, side)], half_h, hs_sem.at[k, side])

    def load_w(d):
        return pltpu.make_async_copy(w_hbm.at[rows_at(d * dt, dt)], a_w.at[rows_at(d * dt, dt)], w_sem.at[d])

    barrier = pltpu.get_barrier_semaphore()
    for step in range(1, n_dev):
        pl.semaphore_signal(barrier, inc=1, device_id=peer(step), device_id_type=MESH)
    each(nr, lambda v: load_h(v).start())
    for k in range(NS):
        for side in range(rows):
            load_s(k, side).start()
    load_w(0).start()
    load_c(0).start()
    sh_acc[...] = jnp.zeros_like(sh_acc)

    def start_h(v):
        load_h(v).wait()
        h_bf[v] = a_h[v].astype(BF16)
        h_t[words_at(v), :] = h_bf[v].T
        own = a_h[v, own_k]
        h_f[v] = own
        sh_acc[own_k, :] += fold_lanes(own)
        load_w(v + 1).start()
        load_c(v + 1).start()

    each(nr, start_h)
    for d in range(nr + 1, ND):
        load_w(d).start()
        load_c(d).start()
    for k in range(NS):
        for side in range(rows):
            load_s(k, side).wait()
            h_bf[NV - 1 - k, :, side * vh:(side + 1) * vh] = (a_o, r_o)[side][k].astype(BF16)
        h_t[words_at(NV - 1 - k), :] = h_bf[NV - 1 - k].T
        own = jnp.where(y == 0, a_o[k], r_o[k])
        h_s[k] = own
        sh_acc[...] += fold_lanes(own)

    pl.semaphore_wait(barrier, n_dev - 1)
    send_sh()
    each(ND, lambda d: copy_c(0, d).start())

    def start_w(d):
        load_w(d).wait()
        w_bf[rows_at(d * dt, dt), :] = a_w[rows_at(d * dt, dt), :].astype(BF16)
        w_f[rows_at(d * quarter, quarter), :] = a_w[mine(d), :]
        load_c(d).wait()

    def sweep_body(sweep, carry):
        last = sweep == SWEEPS - 1

        def s0(d):
            @pl.when(sweep == 0)
            def _():
                start_w(d)
                for v in range(NV):
                    w_tile(d, v)

            @pl.when(sweep > 0)
            def _():
                w_tile(d, nr - 1)
            copy_a(d).start()

            for when, (base, count) in PIECES.items():
                @pl.when(jnp.logical_and(sweep == when, d < count))
                def _(base=base):
                    piece = base + d
                    copy_c(1 + piece // ND, piece % ND).start()

        def s1(d):
            copy_a(d).wait_recv()
            own = rows_at(d * dt + core * half, half)
            a_w[own, :] += r_a[rows_at(d * half, half), :]
            copy_x(d).start()

        def s2(d):
            @pl.when(d == 0)
            def _():
                take_sh()
                sw_acc[...] = jnp.zeros_like(sw_acc)
            copy_x(d).wait_recv()
            own = rows_at(d * quarter, quarter)
            fresh = w_f[own, :] * (a_w[mine(d), :] + r_x[own, :]) / sh_row[0:1, :]
            w_f[own, :] = fresh
            w_bf[mine(d), :] = fresh.astype(BF16)
            copy_g(d).start()
            copy_p(d).start()

            @pl.when(sweep > 0)
            def _():
                copy_u(d).start()

            sw_acc[...] += jnp.sum(fresh.reshape(quarter // 8, 8, topics), axis=0)

            @pl.when(d == ND - 1)
            def _():
                send_sw()

        def s3(d):
            copy_g(d).wait_recv()
            copy_q(d).start()

        def s5(d):
            copy_p(d).wait_recv()
            copy_q(d).wait_recv()
            w_t[...] = w_bf[rows_at(d * dt, dt), :].T

            @pl.when(d < ND - 1)
            def _():
                for v in range(nr):
                    h_tile(d, v)

            @pl.when(d == ND - 1)
            def _():
                h_tile(d, 0)
                h_tile(d, 1)
                copy_y(0).start()
                copy_y(1).start()
                for v in range(2, nr):
                    h_tile(d, v)

        def stage(it, lag, body):
            @pl.when(jnp.logical_and(it >= lag, it < lag + ND))
            def _():
                body(it - lag)

        def w_step(it):
            for lag, body in ((LAG2, s2), (LAG1, s1), (0, s0), (LAG3, s3), (LAG5, s5)):
                stage(it, lag, body)

        each(ND + LAG5, w_step)

        def w_sent(d):
            copy_a(d).wait_send()
            copy_x(d).wait_send()
            copy_g(d).wait_send()
            copy_p(d).wait_send()
            copy_q(d).wait_send()

        each(ND, w_sent)

        def give(d):
            out_w(d).start()
            for step in range(1, cols):
                copy_wo(d, step).start()

        def t1(v):
            @pl.when(v == 0)
            def _():
                take_sw()
                sh_acc[...] = jnp.zeros_like(sh_acc)
            copy_y(v).wait_recv()
            for g in range(vt // LANES):
                at = slice(g * LANES, (g + 1) * LANES)
                fresh = h_f[v, :, at] * (a_h[v, own_k, at] + r_y[v, :, at]) / sw_col[own_k, :]
                h_f[v, :, at] = fresh
                h_bf[v, own_k, at] = fresh.astype(BF16)
                sh_acc[own_k, :] += fresh

            @pl.when(jnp.logical_not(last))
            def _():
                copy_z(v).start()

            @pl.when(last)
            def _():
                out_h(v).start()
                copy_ho(v).start()

            @pl.when(v + 2 < nr)
            def _():
                copy_y(v + 2).start()

        def w_words(v):
            def group(n):
                for k in range(GROUP):
                    w_tile(n * GROUP + k, v)
            each(ND // GROUP, group)

        def t3(v):
            copy_z(v).wait_recv()
            h_t[words_at(v), :] = h_bf[v].T

            @pl.when(v < nr - 1)
            def _():
                w_words(v)

        def update_s(k):
            for g in range(vh // LANES):
                at = slice(g * LANES, (g + 1) * LANES)
                fresh = h_s[k, :, at] * a_s[k, :, at] / sw_col[...]
                h_s[k, :, at] = fresh
                sh_acc[...] += fresh
            h_bf[NV - 1 - k, :, shared(y)] = h_s[k].astype(BF16)

            @pl.when(jnp.logical_not(last))
            def _():
                copy_zs(k).start()

            @pl.when(last)
            def _():
                out_s(k).start()
                copy_hs(k).start()

        def whole_sum(k):
            @pl.when(sweep <= k)
            def _():
                copy_o(k).wait()
                a_s[k] += r_o[k]

            @pl.when(sweep > k)
            def _():
                @pl.when(sweep == k + 1)
                def _():
                    each(ND, lambda d: copy_c(k, d).wait())
                each(ND, lambda d: s_other(k, d))

        def h_step(it):
            @pl.when(it < nr)
            def _():
                t1(it)

            @pl.when(jnp.logical_and(it == 0, sweep > 0))
            def _():
                each(ND, lambda d: copy_u(d).wait_recv())
                for step in range(1, cols):
                    copy_b(step).start()

                @pl.when(last)
                def _():
                    each(ND, give)

            @pl.when(jnp.logical_and(it == S_OTHER, sweep > 0))
            def _():
                for step in range(1, cols):
                    copy_b(step).wait()

            @pl.when(it == 1)
            def _():
                for k in range(2, NS):
                    each(ND, lambda d: s_own(k, d))

            @pl.when(it == S_OTHER)
            def _():
                for k in range(NS - 1):
                    whole_sum(k)

            @pl.when(it == nr - 1)
            def _():
                whole_sum(NS - 1)
                for k in range(NS):
                    update_s(k)

                @pl.when(jnp.logical_not(last))
                def _():
                    send_sh()

            @pl.when(jnp.logical_and(it >= 1, jnp.logical_not(last)))
            def _():
                t3(it - 1)

            @pl.when(jnp.logical_and(it == nr - 1, jnp.logical_not(last)))
            def _():
                for k in range(NS):
                    copy_zs(k).wait_recv()
                    h_t[words_at(NV - 1 - k), :] = h_bf[NV - 1 - k].T
                    w_words(NV - 1 - k)

        for k in range(NS):
            @pl.when(sweep <= k)
            def _(k=k):
                each(ND, lambda d: s_cross(k, d))
                copy_o(k).start()

        for k in range(2):
            each(ND, lambda d: s_own(k, d))
        each(nr + 1, h_step)

        def h_sent(v):
            copy_y(v).wait_send()

            @pl.when(jnp.logical_not(last))
            def _():
                copy_z(v).wait_send()

        each(nr, h_sent)
        @pl.when(sweep > 0)
        def _():
            each(ND, lambda d: copy_u(d).wait_send())

        @pl.when(jnp.logical_not(last))
        def _():
            for k in range(NS):
                copy_zs(k).wait_send()
        return carry

    lax.fori_loop(0, SWEEPS, sweep_body, 0)

    def finish_w(d):
        out_w(d).wait()
        for step in range(1, cols):
            copy_wo(d, step).wait()

    def finish_h(v):
        out_h(v).wait()
        copy_ho(v).wait()

    each(ND, finish_w)
    each(nr, finish_h)
    for k in range(NS):
        out_s(k).wait()
        copy_hs(k).wait()


def solution(mesh):
    rows, cols = mesh.shape["row"], mesh.shape["col"]
    n_dev = rows * cols

    def local(c_blk, w_loc, h_loc):
        docs, words = c_blk.shape
        topics = w_loc.shape[1]
        vmem = pltpu.VMEM
        dma = pltpu.SemaphoreType.DMA
        chunk = words // NV
        scratch = [
            vmem((docs, words), BF16),
            vmem((docs, topics), BF16),
            vmem((topics, docs // ND), BF16),
            vmem((NV, topics, chunk), BF16),
            vmem((words, topics), BF16),
            vmem((docs // 4, topics), F32),
            vmem((NV - NS, topics // 2, chunk), F32),
            vmem((docs, topics), F32),
            vmem((NV - NS, topics, chunk), F32),
            vmem((docs // 2, topics), F32),
            vmem((docs // 4, topics), F32),
            vmem((NV - NS, topics // 2, chunk), F32),
            vmem((8, topics), F32),
            vmem((n_dev, 8, topics), F32),
            vmem((topics, LANES), F32),
            vmem((topics, LANES), F32),
            vmem((8, topics), F32),
            vmem((n_dev, 8, topics), F32),
            vmem((8, topics), F32),
            vmem((NS, docs, chunk // 2), BF16),
            vmem((ND, 4, docs // ND // 4, topics), BF16),
            vmem((NS, topics, chunk // 2), F32),
            vmem((NS, topics, chunk // 2), F32),
        ]
        sizes = [(NS, ND)] * 2 + [ND, ND, cols - 1, cols - 1, (NS, 4), NS, ND, NV, (NS, rows), ND]
        sizes += [ND] * 10 + [NV] * 4 + [n_dev - 1] * 4 + [ND * (cols - 1)] * 2 + [NV] * 2 + [ND, NV]
        scratch += [dma(size if isinstance(size, tuple) else (size,)) for size in sizes]
        extra = [vmem((NS, topics, chunk // 2), F32), vmem((NS, topics, chunk // 2), F32), dma((NS, 2))]
        scratch[31:31] = extra
        any_space = pl.BlockSpec(memory_space=pl.ANY)
        return pl.pallas_call(
            functools.partial(kernel, rows, cols),
            out_shape=(jax.ShapeDtypeStruct(w_loc.shape, F32), jax.ShapeDtypeStruct(h_loc.shape, F32)),
            in_specs=[any_space] * 3,
            out_specs=(any_space, any_space),
            scratch_shapes=scratch,
            compiler_params=pltpu.CompilerParams(
                collective_id=0, has_side_effects=True, vmem_limit_bytes=67_043_328),
            name="nmf",
        )(c_blk, w_loc, h_loc)

    spec_c = P(("part", "row"), "col")
    spec_w = P(("part", "row"), None)
    spec_h = P(None, ("part", "col"))
    return jax.shard_map(local, mesh=mesh, in_specs=(spec_c, spec_w, spec_h), out_specs=(spec_w, spec_h), check_vma=False)
```

```python
import functools

import jax
import jax.numpy as jnp
from jax import lax
from jax.experimental import pallas as pl
from jax.experimental.pallas import tpu as pltpu
from jax.sharding import PartitionSpec as P

SWEEPS = 4
EPS = 1e-6
ND = 8
NV = 8
GROUP = 4
NS = 2
S_OTHER = 3
LAG1, LAG2, LAG3, LAG5 = 2, 4, 5, 7
LANES = 128
MESH = pl.DeviceIdType.MESH
F32 = jnp.float32
BF16 = jnp.bfloat16


def kernel(
    rows, cols, c_hbm, w_hbm, h_hbm, w_out, h_out,
    c_v, w_bf, w_t, h_bf, h_t, w_f, h_f, a_w, a_h, r_a, r_x, r_y,
    sw_acc, sw_slots, sw_col, sh_acc, sh_part, sh_slots, sh_row,
    c_two, w_two, a_s, h_s, c_send, c_recv, u_send, u_recv, b_send, b_recv, s_sems, os_sem,
    a_o, r_o, o_sems,
    w_sem, h_sem, c_sem,
    a_send, a_recv, x_send, x_recv, g_send, g_recv, p_send, p_recv, q_send, q_recv,
    y_send, y_recv, z_send, z_recv, sw_send, sw_recv, sh_send, sh_recv,
    wo_send, wo_recv, ho_send, ho_recv, ow_sem, oh_sem,
):
    docs, words = c_v.shape
    topics = w_bf.shape[1]
    dt, vt, kh = docs // ND, words // NV, topics // 2
    half, quarter = dt // 2, dt // 4
    nr, vh = NV - NS, vt // 2
    n_dev = rows * cols
    y, i = lax.axis_index("row"), lax.axis_index("col")
    x, core = i // 2, i % 2
    me = y * cols + i
    partner = {"col": x * 2 + (1 - core)}
    across = {"col": (1 - x) * 2 + core}
    above = {"row": 1 - y}

    def peer(step):
        other = (me + step) % n_dev
        return {"row": other // cols, "col": other % cols}

    def rows_at(start, size):
        return pl.ds(pl.multiple_of(start, size), size)

    def remote(src, dst, send, recv, device):
        return pltpu.make_async_remote_copy(
            src_ref=src, dst_ref=dst, send_sem=send, recv_sem=recv, device_id=device, device_id_type=MESH)

    def mine(d):
        return rows_at(d * dt + core * half + x * quarter, quarter)

    def theirs(d):
        return rows_at(d * dt + core * half + (1 - x) * quarter, quarter)

    def copy_a(d):
        return remote(a_w.at[rows_at(d * dt + (1 - core) * half, half)], r_a.at[rows_at(d * half, half)],
                      a_send.at[d], a_recv.at[d], partner)

    def copy_x(d):
        return remote(a_w.at[theirs(d)], r_x.at[rows_at(d * quarter, quarter)], x_send.at[d], x_recv.at[d], across)

    def copy_g(d):
        return remote(w_bf.at[mine(d)], w_bf.at[mine(d)], g_send.at[d], g_recv.at[d], across)

    def copy_p(d):
        return remote(w_bf.at[mine(d)], w_bf.at[mine(d)], p_send.at[d], p_recv.at[d], partner)

    def copy_q(d):
        return remote(w_bf.at[theirs(d)], w_bf.at[theirs(d)], q_send.at[d], q_recv.at[d], partner)

    own_k, other_k = rows_at(y * kh, kh), rows_at((1 - y) * kh, kh)

    def words_at(v):
        return rows_at(v * vt, vt)

    def copy_y(v):
        return remote(a_h.at[v, other_k], r_y.at[v], y_send.at[v], y_recv.at[v], above)

    def copy_z(v):
        return remote(h_bf.at[v, own_k], h_bf.at[v, own_k], z_send.at[v], z_recv.at[v], above)

    def shared(side):
        return rows_at(side * vh, vh)

    def whole(k, side):
        return rows_at((NV - 1 - k) * vt + side * vh, vh)

    def copy_c(k, d):
        at = rows_at(d * dt, dt)
        return remote(c_hbm.at[at, whole(k, 1 - y)], c_two.at[k, at], c_send.at[k, d], c_recv.at[k, d], above)

    def copy_o(k):
        return remote(a_o.at[k], r_o.at[k], o_sems.at[k, 0], o_sems.at[k, 1], above)

    def copy_u(d):
        return remote(w_bf.at[mine(d)], w_two.at[d, core * 2 + x], u_send.at[d], u_recv.at[d], above)

    def copy_b(step):
        strip = w_two.at[:, core * 2 + x]
        return remote(strip, strip, b_send.at[step - 1], b_recv.at[step - 1], {"col": (i + step) % cols})

    def copy_zs(k):
        part = h_bf.at[NV - 1 - k, :, shared(y)]
        return remote(part, part, s_sems.at[k, 0], s_sems.at[k, 1], above)

    def copy_hs(k):
        return remote(h_s.at[k], h_out.at[:, whole(k, y)], s_sems.at[k, 2], s_sems.at[k, 3], above)

    def out_s(k):
        return pltpu.make_async_copy(h_s.at[k], h_out.at[:, whole(k, y)], os_sem.at[k])

    def copy_sw(step):
        return remote(sw_acc, sw_slots.at[me], sw_send.at[step - 1], sw_recv.at[step - 1], peer(step))

    def copy_sh(step):
        return remote(sh_part, sh_slots.at[me], sh_send.at[step - 1], sh_recv.at[step - 1], peer(step))

    def copy_wo(d, step):
        k = d * (cols - 1) + step - 1
        return remote(w_f.at[rows_at(d * quarter, quarter)], w_out.at[mine(d)], wo_send.at[k], wo_recv.at[k],
                      {"col": (i + step) % cols})

    def copy_ho(v):
        return remote(h_f.at[v], h_out.at[own_k, words_at(v)], ho_send.at[v], ho_recv.at[v], above)

    def out_w(d):
        return pltpu.make_async_copy(w_f.at[rows_at(d * quarter, quarter)], w_out.at[mine(d)], ow_sem.at[d])

    def out_h(v):
        return pltpu.make_async_copy(h_f.at[v], h_out.at[own_k, words_at(v)], oh_sem.at[v])

    def load_c(d):
        return pltpu.make_async_copy(c_hbm.at[rows_at(d * dt, dt)], c_v.at[rows_at(d * dt, dt)], c_sem.at[d])

    def each(count, body):
        def step(n, carry):
            body(n)
            return carry
        lax.fori_loop(0, count, step, 0)

    def ratio(d, v):
        z = jnp.dot(w_bf[rows_at(d * dt, dt), :], h_bf[v], preferred_element_type=F32)
        return (c_v[rows_at(d * dt, dt), words_at(v)].astype(F32) / (z + EPS)).astype(BF16)

    def select(first, held):
        if isinstance(first, bool):
            return jnp.zeros_like(held) if first else held
        return jnp.where(first, 0.0, held)

    def w_tile(d, v):
        part = jnp.dot(ratio(d, v), h_t[words_at(v), :], preferred_element_type=F32)
        held = a_w[rows_at(d * dt, dt), :]
        a_w[rows_at(d * dt, dt), :] = select(v == 0, held) + part

    def h_tile(d, v):
        part = jnp.dot(w_t[...], ratio(d, v), preferred_element_type=F32)
        held = a_h[v]
        a_h[v] = select(d == 0, held) + part

    def s_tile(total, rows_bf, counts, h_half, first):
        z = jnp.dot(rows_bf, h_half, preferred_element_type=F32)
        q = (counts.astype(F32) / (z + EPS)).astype(BF16)
        part = jnp.dot(rows_bf.T, q, preferred_element_type=F32)
        total[...] = jnp.where(first, 0.0, total[...]) + part

    def s_own(k, d):
        at = rows_at(d * dt, dt)
        s_tile(a_s.at[k], w_bf[at, :], c_v[at, whole(k, y)], h_bf[NV - 1 - k, :, shared(y)], d == 0)

    def s_cross(k, d):
        at = rows_at(d * dt, dt)
        s_tile(a_o.at[k], w_bf[at, :], c_v[at, whole(k, 1 - y)], h_bf[NV - 1 - k, :, shared(1 - y)], d == 0)

    def s_other(k, d):
        counts = c_two[k, rows_at(d * dt, dt), :]
        s_tile(a_s.at[k], w_two[d].reshape(dt, topics), counts, h_bf[NV - 1 - k, :, shared(y)], False)

    def fold_lanes(block):
        total = block[:, :LANES]
        for g in range(1, block.shape[1] // LANES):
            total = total + block[:, g * LANES:(g + 1) * LANES]
        return total

    def send_sh():
        for r in range(rows):
            at = slice(r * kh, (r + 1) * kh)
            sh_part[:, at] = jnp.sum(sh_acc[at, :].T.reshape(LANES // 8, 8, kh), axis=0)
        sh_slots[me] = sh_part[...]
        for step in range(1, n_dev):
            copy_sh(step).start()

    def take_sh():
        for step in range(1, n_dev):
            copy_sh(step).wait()
        total = sh_slots[0]
        for n in range(1, n_dev):
            total = total + sh_slots[n]
        sh_row[...] = jnp.broadcast_to(jnp.sum(total, axis=0, keepdims=True), (8, topics))

    def send_sw():
        sw_slots[me] = sw_acc[...]
        for step in range(1, n_dev):
            copy_sw(step).start()

    def take_sw():
        for step in range(1, n_dev):
            copy_sw(step).wait()
        total = sw_slots[0]
        for n in range(1, n_dev):
            total = total + sw_slots[n]
        total = jnp.sum(total, axis=0, keepdims=True)
        for r in range(rows):
            at = slice(r * kh, (r + 1) * kh)
            sw_col[at, :] = jnp.broadcast_to(total[:, at], (LANES, kh)).T

    def load_h(v):
        return pltpu.make_async_copy(h_hbm.at[:, words_at(v)], a_h.at[v], h_sem.at[v])

    def load_w(d):
        return pltpu.make_async_copy(w_hbm.at[rows_at(d * dt, dt)], a_w.at[rows_at(d * dt, dt)], w_sem.at[d])

    barrier = pltpu.get_barrier_semaphore()
    for step in range(1, n_dev):
        pl.semaphore_signal(barrier, inc=1, device_id=peer(step), device_id_type=MESH)
    each(NV, lambda v: load_h(v).start())
    load_w(0).start()
    load_c(0).start()
    sh_acc[...] = jnp.zeros_like(sh_acc)

    def start_h(v):
        load_h(v).wait()
        h_bf[v] = a_h[v].astype(BF16)
        h_t[words_at(v), :] = h_bf[v].T

        @pl.when(v < nr)
        def _():
            own = a_h[v, own_k]
            h_f[v] = own
            sh_acc[own_k, :] += fold_lanes(own)

        @pl.when(v >= nr)
        def _():
            own = a_h[v, :, shared(y)]
            h_s[NV - 1 - v] = own
            sh_acc[...] += fold_lanes(own)

        @pl.when(v + 1 < ND)
        def _():
            load_w(v + 1).start()
            load_c(v + 1).start()

    each(NV, start_h)
    pl.semaphore_wait(barrier, n_dev - 1)
    send_sh()
    each(ND, lambda d: copy_c(0, d).start())

    def start_w(d):
        load_w(d).wait()
        w_bf[rows_at(d * dt, dt), :] = a_w[rows_at(d * dt, dt), :].astype(BF16)
        w_f[rows_at(d * quarter, quarter), :] = a_w[mine(d), :]
        load_c(d).wait()

    def sweep_body(sweep, carry):
        last = sweep == SWEEPS - 1

        def s0(d):
            @pl.when(sweep == 0)
            def _():
                start_w(d)
                for v in range(NV):
                    w_tile(d, v)

            @pl.when(sweep > 0)
            def _():
                w_tile(d, nr - 1)
            copy_a(d).start()

        def s1(d):
            copy_a(d).wait_recv()
            own = rows_at(d * dt + core * half, half)
            a_w[own, :] += r_a[rows_at(d * half, half), :]
            copy_x(d).start()

        def s2(d):
            @pl.when(d == 0)
            def _():
                take_sh()
                sw_acc[...] = jnp.zeros_like(sw_acc)
            copy_x(d).wait_recv()
            own = rows_at(d * quarter, quarter)
            fresh = w_f[own, :] * (a_w[mine(d), :] + r_x[own, :]) / sh_row[0:1, :]
            w_f[own, :] = fresh
            w_bf[mine(d), :] = fresh.astype(BF16)
            copy_g(d).start()
            copy_p(d).start()

            @pl.when(sweep > 0)
            def _():
                copy_u(d).start()

            for k in range(1, NS):
                @pl.when(jnp.logical_and(jnp.logical_or(sweep == k, sweep == k + 1), d < ND // 2))
                def _(k=k):
                    copy_c(k, (sweep - k) * (ND // 2) + d).start()
            sw_acc[...] += jnp.sum(fresh.reshape(quarter // 8, 8, topics), axis=0)

            @pl.when(d == ND - 1)
            def _():
                send_sw()

        def s3(d):
            copy_g(d).wait_recv()
            copy_q(d).start()

        def s5(d):
            copy_p(d).wait_recv()
            copy_q(d).wait_recv()
            w_t[...] = w_bf[rows_at(d * dt, dt), :].T

            @pl.when(d < ND - 1)
            def _():
                for v in range(nr):
                    h_tile(d, v)

            @pl.when(d == ND - 1)
            def _():
                h_tile(d, 0)
                h_tile(d, 1)
                copy_y(0).start()
                copy_y(1).start()
                for v in range(2, nr):
                    h_tile(d, v)

        def stage(it, lag, body):
            @pl.when(jnp.logical_and(it >= lag, it < lag + ND))
            def _():
                body(it - lag)

        def w_step(it):
            for lag, body in ((LAG5, s5), (LAG2, s2), (LAG1, s1), (0, s0), (LAG3, s3)):
                stage(it, lag, body)

        each(ND + LAG5, w_step)

        def w_sent(d):
            copy_a(d).wait_send()
            copy_x(d).wait_send()
            copy_g(d).wait_send()
            copy_p(d).wait_send()
            copy_q(d).wait_send()

        each(ND, w_sent)

        def give(d):
            out_w(d).start()
            for step in range(1, cols):
                copy_wo(d, step).start()

        def t1(v):
            @pl.when(v == 0)
            def _():
                take_sw()
                sh_acc[...] = jnp.zeros_like(sh_acc)
            copy_y(v).wait_recv()
            for g in range(vt // LANES):
                at = slice(g * LANES, (g + 1) * LANES)
                fresh = h_f[v, :, at] * (a_h[v, own_k, at] + r_y[v, :, at]) / sw_col[own_k, :]
                h_f[v, :, at] = fresh
                h_bf[v, own_k, at] = fresh.astype(BF16)
                sh_acc[own_k, :] += fresh

            @pl.when(jnp.logical_not(last))
            def _():
                copy_z(v).start()

                @pl.when(v == nr - 1)
                def _():
                    send_sh()

            @pl.when(last)
            def _():
                out_h(v).start()
                copy_ho(v).start()

            @pl.when(v + 2 < nr)
            def _():
                copy_y(v + 2).start()

        def w_words(v):
            def group(n):
                for k in range(GROUP):
                    w_tile(n * GROUP + k, v)
            each(ND // GROUP, group)

        def t3(v):
            copy_z(v).wait_recv()
            h_t[words_at(v), :] = h_bf[v].T

            @pl.when(v < nr - 1)
            def _():
                w_words(v)

        def update_s(k):
            for g in range(vh // LANES):
                at = slice(g * LANES, (g + 1) * LANES)
                fresh = h_s[k, :, at] * a_s[k, :, at] / sw_col[...]
                h_s[k, :, at] = fresh
                sh_acc[...] += fresh
            h_bf[NV - 1 - k, :, shared(y)] = h_s[k].astype(BF16)

            @pl.when(jnp.logical_not(last))
            def _():
                copy_zs(k).start()

            @pl.when(last)
            def _():
                out_s(k).start()
                copy_hs(k).start()

        def whole_sum(k):
            @pl.when(sweep <= k)
            def _():
                copy_o(k).wait()
                a_s[k] += r_o[k]

            @pl.when(sweep > k)
            def _():
                @pl.when(sweep == k + 1)
                def _():
                    each(ND, lambda d: copy_c(k, d).wait())
                each(ND, lambda d: s_other(k, d))

        def h_step(it):
            @pl.when(it < nr)
            def _():
                t1(it)

            @pl.when(jnp.logical_and(it == 0, sweep > 0))
            def _():
                each(ND, lambda d: copy_u(d).wait_recv())
                for step in range(1, cols):
                    copy_b(step).start()

                @pl.when(last)
                def _():
                    each(ND, give)

            @pl.when(jnp.logical_and(it == S_OTHER, sweep > 0))
            def _():
                for step in range(1, cols):
                    copy_b(step).wait()

            for k in range(NS):
                @pl.when(it == S_OTHER + k)
                def _(k=k):
                    whole_sum(k)

            @pl.when(it == S_OTHER + NS - 1)
            def _():
                for k in range(NS):
                    update_s(k)

            @pl.when(jnp.logical_and(it >= 1, jnp.logical_not(last)))
            def _():
                t3(it - 1)

            @pl.when(jnp.logical_and(it == nr - 1, jnp.logical_not(last)))
            def _():
                for k in range(NS):
                    copy_zs(k).wait_recv()
                    h_t[words_at(NV - 1 - k), :] = h_bf[NV - 1 - k].T
                    w_words(NV - 1 - k)

        for k in range(NS):
            @pl.when(sweep <= k)
            def _(k=k):
                each(ND, lambda d: s_cross(k, d))
                copy_o(k).start()

        for k in range(NS):
            each(ND, lambda d: s_own(k, d))
        each(nr + 1, h_step)

        def h_sent(v):
            copy_y(v).wait_send()

            @pl.when(jnp.logical_not(last))
            def _():
                copy_z(v).wait_send()

        each(nr, h_sent)
        @pl.when(sweep > 0)
        def _():
            each(ND, lambda d: copy_u(d).wait_send())

        @pl.when(jnp.logical_not(last))
        def _():
            for k in range(NS):
                copy_zs(k).wait_send()
        return carry

    lax.fori_loop(0, SWEEPS, sweep_body, 0)

    def finish_w(d):
        out_w(d).wait()
        for step in range(1, cols):
            copy_wo(d, step).wait()

    def finish_h(v):
        out_h(v).wait()
        copy_ho(v).wait()

    each(ND, finish_w)
    each(nr, finish_h)
    for k in range(NS):
        out_s(k).wait()
        copy_hs(k).wait()


def solution(mesh):
    rows, cols = mesh.shape["row"], mesh.shape["col"]
    n_dev = rows * cols

    def local(c_blk, w_loc, h_loc):
        docs, words = c_blk.shape
        topics = w_loc.shape[1]
        vmem = pltpu.VMEM
        dma = pltpu.SemaphoreType.DMA
        chunk = words // NV
        scratch = [
            vmem((docs, words), BF16),
            vmem((docs, topics), BF16),
            vmem((topics, docs // ND), BF16),
            vmem((NV, topics, chunk), BF16),
            vmem((words, topics), BF16),
            vmem((docs // 4, topics), F32),
            vmem((NV - NS, topics // 2, chunk), F32),
            vmem((docs, topics), F32),
            vmem((NV, topics, chunk), F32),
            vmem((docs // 2, topics), F32),
            vmem((docs // 4, topics), F32),
            vmem((NV - NS, topics // 2, chunk), F32),
            vmem((8, topics), F32),
            vmem((n_dev, 8, topics), F32),
            vmem((topics, LANES), F32),
            vmem((topics, LANES), F32),
            vmem((8, topics), F32),
            vmem((n_dev, 8, topics), F32),
            vmem((8, topics), F32),
            vmem((NS, docs, chunk // 2), BF16),
            vmem((ND, 4, docs // ND // 4, topics), BF16),
            vmem((NS, topics, chunk // 2), F32),
            vmem((NS, topics, chunk // 2), F32),
        ]
        sizes = [(NS, ND)] * 2 + [ND, ND, cols - 1, cols - 1, (NS, 4), NS, ND, NV, ND]
        sizes += [ND] * 10 + [NV] * 4 + [n_dev - 1] * 4 + [ND * (cols - 1)] * 2 + [NV] * 2 + [ND, NV]
        scratch += [dma(size if isinstance(size, tuple) else (size,)) for size in sizes]
        extra = [vmem((NS, topics, chunk // 2), F32), vmem((NS, topics, chunk // 2), F32), dma((NS, 2))]
        scratch[31:31] = extra
        any_space = pl.BlockSpec(memory_space=pl.ANY)
        return pl.pallas_call(
            functools.partial(kernel, rows, cols),
            out_shape=(jax.ShapeDtypeStruct(w_loc.shape, F32), jax.ShapeDtypeStruct(h_loc.shape, F32)),
            in_specs=[any_space] * 3,
            out_specs=(any_space, any_space),
            scratch_shapes=scratch,
            compiler_params=pltpu.CompilerParams(
                collective_id=0, has_side_effects=True, vmem_limit_bytes=67_043_328),
            name="nmf",
        )(c_blk, w_loc, h_loc)

    spec_c = P(("part", "row"), "col")
    spec_w = P(("part", "row"), None)
    spec_h = P(None, ("part", "col"))
    return jax.shard_map(local, mesh=mesh, in_specs=(spec_c, spec_w, spec_h), out_specs=(spec_w, spec_h), check_vma=False)
```
